32 devices in a mesh: gz: 32 (over z, y, x, core).
Axes of the slice: x: 2, y: 2, z: 4, core: 2. Of those that a mesh axis runs over, the one named last changes fastest.
Arguments:
- coefficient: float32 [64, 512, 512], P('gz'), may hold values from 0.2 to 1.3
- initial_field: float32 [64, 512, 512], P('gz'), may hold values from -6 to 6
- observed: float32 [64, 512, 512], P('gz'), may hold values from -6 to 6
- misfit_weight: float32 [64, 512, 512], P('gz'), may hold values from 0.5 to 6, as said below
Outputs:
- coeff_gradient: float32 [64, 512, 512], P('gz')
- adjoint_field: float32 [64, 512, 512], P('gz')
- misfit: float32 [], replicated
The draws below stay inside these ranges and needn't reach their ends.
Inputs may be any that keep to these rules, and one draw needn't show every extreme that they name: `misfit_weight`: positive cell weights.
All inputs are finite; a program needn't handle non-finite values.
Results may differ from the reference program's by a relative error of at most 0.00002.
Values sent between devices are 32-bit elements; how exact they have to be, the bound alone decides.
A program may use at most 128 MiB of HBM per device.

```python
import math
import jax
import jax.numpy as jnp

NY = 512
NX = 512
ITERS = 4
NZ = 64


def draw_misfit_weight(key, part):
    depth = jnp.arange(NZ, dtype=jnp.float32)[:, None, None]
    ramp = 1.0 + 2.0 * depth / (NZ - 1)
    base = jnp.exp(jax.random.uniform(key, (NZ, NY, NX), jnp.float32, jnp.log(0.5), jnp.log(2.0)))
    return (ramp * base).astype(jnp.float32)


def block_scale(stream_key, shape, split, smallest, high):
    def one(axis_at, parts):
        steps = jax.random.uniform(jax.random.fold_in(jax.random.fold_in(stream_key, 6), axis_at), (parts,), jnp.float32, smallest / len(split), high / len(split))
        return jnp.repeat(jnp.exp(steps), shape[axis_at] // parts).reshape((-1,) + (1,) * (len(shape) - axis_at - 1))

    gain = one(*split[0])
    for cut in split[1:]:
        gain = gain * one(*cut)
    return gain


def centred(key, extent, width, bound, split=(), kind=jnp.bfloat16):
    array = width * jax.random.normal(key, extent, jnp.float32)
    if split:
        array = array * block_scale(key, extent, split, -0.22, 0.18)
    return jnp.clip(array, -bound, bound).astype(kind)


def setup_inputs(seed: int = 0) -> dict:
    splits = jax.random.split(jax.random.key(seed), 5)
    coefficient = jnp.clip(jnp.exp(math.log(1.3) - 1.8718021 * jax.random.uniform(splits[0], (NZ, NY, NX), jnp.float32) ** block_scale(splits[0], (NZ, NY, NX), ((0, 32),), -0.2, 0.2)), 0.2, 1.3)
    initial_field = centred(splits[1], (NZ, NY, NX), 1.0, 6.0, ((0, 32),), jnp.float32)
    observed = centred(splits[2], (NZ, NY, NX), 1.0, 6.0, ((0, 32),), jnp.float32)
    misfit_weight = draw_misfit_weight(jax.random.fold_in(splits[4], 71), 0)
    return {"coefficient": coefficient, "initial_field": initial_field, "observed": observed, "misfit_weight": misfit_weight}


time_step = 0.125

def laplace(field):
    padded = jnp.pad(field, 1)
    beside = padded[2:, 1:-1, 1:-1] + padded[:-2, 1:-1, 1:-1]
    beside = beside + padded[1:-1, 2:, 1:-1] + padded[1:-1, :-2, 1:-1]
    beside = beside + padded[1:-1, 1:-1, 2:] + padded[1:-1, 1:-1, :-2]
    return beside - 6.0 * field

def reference(coefficient, initial_field, observed, misfit_weight):
    state = initial_field
    slopes = []
    for step in range(ITERS):
        slope = laplace(state)
        slopes.append(slope)
        state = state + time_step * coefficient * slope
    resid = state - observed
    total = jnp.sum(misfit_weight * resid * resid)
    misfit = jnp.sqrt(total / (NZ * NY * NX) + 1e-06)
    adjoint = misfit_weight * resid / misfit
    gradient = jnp.zeros_like(coefficient)
    for step in reversed(range(ITERS)):
        gradient = gradient + time_step * adjoint * slopes[step]
        adjoint = adjoint + time_step * laplace(coefficient * adjoint)
    return (gradient, adjoint, misfit)
```

```python
import functools

import jax
import jax.numpy as jnp
from jax import lax
from jax.experimental import pallas as pl
from jax.experimental.pallas import tpu as pltpu
from jax.sharding import PartitionSpec as P

ITERS = 4
time_step = 0.125
MESH = pl.DeviceIdType.MESH
PAD = 8
TILE = 8
CHUNKS = 16


def kernel(n, rounds, cells, coef_hbm, init_hbm, obs_hbm, wgt_hbm, grad_out, adj_out, misfit_out,
           st, sl, halo, coef, obs, wgt, gacc, aacc, acc, part, edge_out, edge_in,
           in_send, in_recv, halo_send, halo_recv, edge_send, edge_recv,
           out_send, out_recv, psend_sem, precv_sem):
    own, ny, nx = coef_hbm.shape
    planes, half = 2 * own, ny // 2
    rows = half // CHUNKS
    exchanges = 2 * ITERS
    me = lax.axis_index("gz")
    q = me % 4
    base = me - q
    h, s = q // 2, q % 2
    lower, upper = me - 3 + 2 * s, me + 1 + 2 * s
    mate = me + 2 - 4 * h
    has_lo = lower >= 0
    has_hi = upper < n
    partners = []
    for r in range(rounds):
        bit = 1 << r
        partners.append(me + bit * (1 - 2 * ((me // bit) % 2)))
    sums = [partners[0]] + partners[2:]
    free = s == h

    barrier = pltpu.get_barrier_semaphore()

    def greet(device):
        pl.semaphore_signal(barrier, inc=1, device_id=(device,), device_id_type=MESH)

    for i in range(1, 4):
        greet(base + (q + i) % 4)
    outside_lo = (s == 0) & has_lo
    outside_hi = (s == 1) & has_hi

    @pl.when(outside_lo)
    def _():
        greet(lower)

    @pl.when(outside_hi)
    def _():
        greet(upper)

    zero_rows = jnp.zeros((PAD, nx), jnp.float32)
    outer = pl.multiple_of(h * (PAD + half), PAD)
    inner = pl.multiple_of((1 - h) * (PAD + half), PAD)

    crossing = outside_lo | outside_hi

    @pl.when(crossing)
    def _():
        pl.semaphore_wait(barrier, 4)

    @pl.when(jnp.logical_not(crossing))
    def _():
        pl.semaphore_wait(barrier, 3)

    hbm = (init_hbm, coef_hbm, obs_hbm, wgt_hbm)
    held = (None, coef, obs, wgt)

    def place(side_half, j):
        return j if side_half == 1 else CHUNKS - 1 - j

    def feed(array, j):
        for to in range(2):
            dest = base + 2 * to + q // 2
            row = place(to, j) * rows
            slot = pl.ds(s * own, own)
            if array == 0:
                src = init_hbm.at[:, pl.ds(pl.multiple_of(to * half + row, PAD), rows), :]
                dst = st.at[0, slot, pl.ds(pl.multiple_of(PAD + row, PAD), rows), :]
            else:
                src = hbm[array].at[:, pl.ds(pl.multiple_of(to * half + row, PAD), rows), :]
                dst = held[array].at[slot, pl.ds(pl.multiple_of(row, PAD), rows), :]
            arrived = in_recv.at[array, s, j]

            @pl.when(dest == me)
            def _():
                pltpu.make_async_copy(src, dst, arrived).start()

            @pl.when(dest != me)
            def _():
                pltpu.make_async_remote_copy(
                    src_ref=src, dst_ref=dst, send_sem=in_send.at[array, to], recv_sem=arrived,
                    device_id=(dest,), device_id_type=MESH,
                ).start()

    def await_copy(ref, sem):
        pltpu.make_async_copy(ref, ref, sem).wait()

    def fed(array, j, at):
        for slot in range(2):
            arrived = in_recv.at[array, slot, j]
            mine = pl.ds(slot * own, own)
            if array == 0:
                await_copy(st.at[0, mine, pl.ds(pl.multiple_of(PAD + at, PAD), rows), :], arrived)
            else:
                await_copy(held[array].at[mine, pl.ds(at, rows), :], arrived)

    for j in range(3):
        feed(0, j)
        feed(1, j)

    def clear_pad(e, carry):
        for p in range(planes):
            st[e, p, pl.ds(outer, PAD), :] = zero_rows
        return carry

    lax.fori_loop(0, exchanges, clear_pad, 0)

    def clear_halo(side):
        def clear(i, carry):
            e = i // (half // PAD)
            row = pl.multiple_of((i % (half // PAD)) * PAD, PAD)
            halo[side, e, pl.ds(row, PAD), :] = zero_rows
            return carry

        lax.fori_loop(0, exchanges * (half // PAD), clear, 0)

    @pl.when(jnp.logical_not(has_lo))
    def _():
        clear_halo(0)

    @pl.when(jnp.logical_not(has_hi))
    def _():
        clear_halo(1)

    acc[...] = jnp.zeros_like(acc)
    def send(e, at, j):
        here = pl.ds(at, rows)
        padded = pl.ds(pl.multiple_of(PAD + at, PAD), rows)

        def copy(side, device):
            pltpu.make_async_remote_copy(
                src_ref=st.at[e, (planes - 1) * (1 - side), padded, :],
                dst_ref=halo.at[side, e, here, :],
                send_sem=halo_send.at[side, e], recv_sem=halo_recv.at[side, e, j],
                device_id=(device,), device_id_type=MESH,
            ).start()

        @pl.when(has_hi)
        def _():
            copy(0, upper)

        @pl.when(has_lo)
        def _():
            copy(1, lower)

    def receive(e, at, j):
        here = pl.ds(at, rows)

        @pl.when(has_lo)
        def _():
            await_copy(halo.at[0, e, here, :], halo_recv.at[0, e, j])

        @pl.when(has_hi)
        def _():
            await_copy(halo.at[1, e, here, :], halo_recv.at[1, e, j])

    def edge_copy(e):
        return pltpu.make_async_remote_copy(
            src_ref=edge_out.at[e], dst_ref=edge_in.at[e],
            send_sem=edge_send.at[e], recv_sem=edge_recv.at[e],
            device_id=(mate,), device_id_type=MESH,
        )

    def stage_edge(e):
        at = pl.multiple_of(PAD + (1 - h) * (half - PAD), PAD)
        for p in range(planes):
            block = st[e, p, pl.ds(at, PAD), :]
            edge_out[e, p:p + 1, :] = jnp.where(h == 0, block[PAD - 1:PAD], block[0:1])

    def take_edge(e):
        edge_copy(e).wait_recv()
        for p in range(planes):
            st[e, p, pl.ds(inner, PAD), :] = jnp.broadcast_to(edge_in[e, p:p + 1, :], (PAD, nx))

    lane = lax.broadcasted_iota(jnp.int32, (TILE, nx), 1)
    leftmost = lane == 0
    rightmost = lane == nx - 1

    def laplace(e, p, row):
        here = pl.ds(row, TILE)
        padded = pl.ds(pl.multiple_of(row + PAD, PAD), TILE)
        tall = st[e, p, pl.ds(row, TILE + 2 * PAD), :]
        mid = tall[PAD:PAD + TILE]
        beside = tall[PAD + 1:PAD + 1 + TILE] + tall[PAD - 1:PAD - 1 + TILE]
        beside = beside + jnp.where(rightmost, 0.0, pltpu.roll(mid, nx - 1, 1))
        beside = beside + jnp.where(leftmost, 0.0, pltpu.roll(mid, 1, 1))
        above = st[e, p + 1, padded, :] if p + 1 < planes else halo[1, e, here, :]
        below = st[e, p - 1, padded, :] if p > 0 else halo[0, e, here, :]
        return mid, beside + above + below - 6.0 * mid

    def ship(which, source, target, m):
        at = pl.multiple_of((CHUNKS - 2 - 2 * m) * (1 - h) * rows + 2 * m * h * rows, PAD)
        for o in range(2):
            dest = base + 2 * s + o
            src = source.at[pl.ds(o * own, own), pl.ds(at, 2 * rows), :]
            dst = target.at[:, pl.ds(pl.multiple_of(h * half + at, PAD), 2 * rows), :]

            @pl.when(dest == me)
            def _():
                pltpu.make_async_copy(src, dst, out_recv.at[which, h]).start()

            @pl.when(dest != me)
            def _():
                pltpu.make_async_remote_copy(
                    src_ref=src, dst_ref=dst, send_sem=out_send.at[which, o],
                    recv_sem=out_recv.at[which, h], device_id=(dest,), device_id_type=MESH,
                ).start()

    def stage(e, j):
        at = pl.multiple_of((CHUNKS - 1 - j) * (1 - h) * rows + j * h * rows, PAD)
        if e == 0:
            fed(1, j, at)

        @pl.when(j == 0)
        def _():
            take_edge(e)

        if e == ITERS - 1:
            fed(2, j, at)
            fed(3, j, at)
        receive(e, at, j)

        def tile(t, carry):
            row = pl.multiple_of(at + t * TILE, TILE)
            here = pl.ds(row, TILE)
            padded = pl.ds(pl.multiple_of(row + PAD, PAD), TILE)
            for p in range(planes):
                mid, slope = laplace(e, p, row)
                if e < ITERS - 1:
                    sl[e, p, here, :] = slope
                    st[e + 1, p, padded, :] = mid + time_step * coef[p, here, :] * slope
                elif e == ITERS - 1:
                    c = coef[p, here, :]
                    resid = mid + time_step * c * slope - obs[p, here, :]
                    weighted = wgt[p, here, :] * resid
                    acc[...] += weighted * resid
                    aacc[p, here, :] = weighted
                    gacc[p, here, :] = time_step * weighted * slope
                    st[e + 1, p, padded, :] = c * weighted
                else:
                    lam = aacc[p, here, :] + time_step * slope
                    aacc[p, here, :] = lam
                    if e < exchanges - 1:
                        gacc[p, here, :] += time_step * lam * sl[exchanges - 2 - e, p, here, :]
                        st[e + 1, p, padded, :] = coef[p, here, :] * lam
            return carry

        lax.fori_loop(0, rows // TILE, tile, 0)
        if e < exchanges - 1:
            @pl.when(j == 0)
            def _():
                stage_edge(e + 1)

            send(e + 1, at, j)

            @pl.when(j == 0)
            def _():
                edge_copy(e + 1).start()

    def exchange(r):
        return pltpu.make_async_remote_copy(
            src_ref=part.at[2 * r], dst_ref=part.at[2 * r + 1],
            send_sem=psend_sem.at[r], recv_sem=precv_sem.at[r],
            device_id=(sums[r],), device_id_type=MESH,
        )

    def across(o):
        return pltpu.make_async_remote_copy(
            src_ref=part.at[2 * rounds - 2], dst_ref=part.at[2 * rounds - 1],
            send_sem=psend_sem.at[rounds - 1 + o], recv_sem=precv_sem.at[rounds - 1],
            device_id=(base + 2 * (1 - h) + o,), device_id_type=MESH,
        )

    def total_round(r):
        if r == 0:
            whole = acc[...]
            narrow = whole[:, 0:128]
            for i in range(1, nx // 128):
                narrow = narrow + whole[:, 128 * i:128 * i + 128]
            part[0] = narrow
        else:
            exchange(r - 1).wait_recv()
            part[2 * r] = part[2 * r - 2] + part[2 * r - 1]
        if r < rounds - 1:
            exchange(r).start()
        else:
            @pl.when(free)
            def _():
                across(0).start()
                across(1).start()

    summed = CHUNKS + ITERS - 1
    ticks = CHUNKS + exchanges

    def tick(t, carry):
        @pl.when(t < CHUNKS)
        def _():
            at = pl.multiple_of((CHUNKS - 1 - t) * (1 - h) * rows + t * h * rows, PAD)
            fed(0, t, at)

            @pl.when(t == 0)
            def _():
                stage_edge(0)
                edge_copy(0).start()

            send(0, at, t)

        for e in range(exchanges):
            j = t - 1 - e

            @pl.when((j >= 0) & (j < CHUNKS))
            def _():
                stage(e, j)

        @pl.when(t + 3 < CHUNKS)
        def _():
            feed(0, t + 3)
            feed(1, t + 3)

        late = t + 2 - ITERS + 1

        @pl.when((late >= 0) & (late < CHUNKS))
        def _():
            feed(2, late)
            feed(3, late)

        for which, source, target, begin in ((0, gacc, grad_out, CHUNKS - 2), (1, aacc, adj_out, CHUNKS - 1)):
            m, final = t - begin, CHUNKS // 2 - 1

            @pl.when((m >= 0) & (m < final))
            def _():
                ship(which, source, target, m)

            @pl.when(m == final + 1)
            def _():
                ship(which, source, target, final)

        for r in range(min(rounds, ticks - summed)):
            @pl.when(t == summed + r)
            def _():
                total_round(r)

        return carry

    lax.fori_loop(0, ticks, tick, 0)
    for r in range(ticks - summed, rounds):
        total_round(r)

    across(0).wait_recv()
    whole = part[2 * rounds - 2] + part[2 * rounds - 1]
    whole = jnp.sum(jnp.sum(whole, axis=1, keepdims=True), axis=0, keepdims=True)
    misfit_out[...] = jnp.sqrt(jnp.broadcast_to(whole, (8, 128)) / cells + 1e-06)

    for which, target in enumerate((grad_out, adj_out)):
        for side in range(2):
            await_copy(target.at[:, pl.ds(side * half, half), :], out_recv.at[which, side])
    for which, source in enumerate((gacc, aacc)):
        for o in range(2):
            @pl.when(base + 2 * s + o != me)
            def _():
                await_copy(source.at[pl.ds(o * own, own)], out_send.at[which, o])
    for array in range(4):
        for to in range(2):
            @pl.when(base + 2 * to + q // 2 != me)
            def _():
                await_copy(hbm[array].at[:, pl.ds(0, half), :], in_send.at[array, to])
    for e in range(exchanges):
        @pl.when(has_hi)
        def _():
            await_copy(halo.at[0, e], halo_send.at[0, e])

        @pl.when(has_lo)
        def _():
            await_copy(halo.at[1, e], halo_send.at[1, e])
    for e in range(exchanges):
        edge_copy(e).wait_send()
    for r in range(rounds - 1):
        exchange(r).wait_send()

    @pl.when(free)
    def _():
        across(0).wait_send()
        across(1).wait_send()


def solution(mesh):
    n = mesh.shape["gz"]
    rounds = n.bit_length() - 1

    def on_device(coefficient, initial_field, observed, misfit_weight):
        own, ny, nx = coefficient.shape
        planes, half = 2 * own, ny // 2
        slab = jax.ShapeDtypeStruct(coefficient.shape, jnp.float32)
        exchanges = 2 * ITERS
        block = pltpu.VMEM((planes, half, nx), jnp.float32)
        edge = pltpu.VMEM((exchanges, planes, nx), jnp.float32)
        dma = pltpu.SemaphoreType.DMA
        grad, adj, misfit = pl.pallas_call(
            functools.partial(kernel, n, rounds, float(n * own * ny * nx)),
            out_shape=(slab, slab, jax.ShapeDtypeStruct((8, 128), jnp.float32)),
            in_specs=[pl.BlockSpec(memory_space=pl.ANY)] * 4,
            out_specs=[pl.BlockSpec(memory_space=pl.ANY)] * 2 + [pl.BlockSpec(memory_space=pltpu.VMEM)],
            scratch_shapes=[
                pltpu.VMEM((exchanges, planes, half + 2 * PAD, nx), jnp.float32),
                pltpu.VMEM((ITERS - 1, planes, half, nx), jnp.float32),
                pltpu.VMEM((2, exchanges, half, nx), jnp.float32),
                block, block, block, block, block,
                pltpu.VMEM((TILE, nx), jnp.float32),
                pltpu.VMEM((2 * rounds, 8, 128), jnp.float32),
                edge, edge,
                dma((4, 2)), dma((4, 2, CHUNKS)),
                dma((2, exchanges)), dma((2, exchanges, CHUNKS)),
                dma((exchanges,)), dma((exchanges,)),
                dma((2, 2)), dma((2, 2)),
                dma((rounds + 1,)), dma((rounds,)),
            ],
            compiler_params=pltpu.CompilerParams(
                collective_id=0, has_side_effects=True, vmem_limit_bytes=48 * 1024 * 1024
            ),
        )(coefficient, initial_field, observed, misfit_weight)
        scale = misfit[0, 0]
        return grad / scale, adj / scale, scale

    placed = P("gz", None, None)
    return jax.shard_map(
        on_device,
        mesh=mesh,
        in_specs=(placed,) * 4,
        out_specs=(placed, placed, P()),
        check_vma=False,
    )
```

```python
import functools

import jax
import jax.numpy as jnp
from jax import lax
from jax.experimental import pallas as pl
from jax.experimental.pallas import tpu as pltpu
from jax.sharding import PartitionSpec as P

ITERS = 4
time_step = 0.125
MESH = pl.DeviceIdType.MESH
PAD = 8
TILE = 8
CHUNKS = 16
RING = 4
PIECE = 128


def kernel(n, rounds, cells, coef_hbm, init_hbm, obs_hbm, wgt_hbm, grad_out, adj_out, misfit_out,
           st, sl, halo, coef, obs, wgt, gacc, aacc, acc, part, edge_out, edge_in,
           in_send, in_recv, halo_send, halo_recv, edge_send, edge_recv,
           out_send, out_recv, psend_sem, precv_sem, first, first_sem):
    own, ny, nx = coef_hbm.shape
    planes, half = 2 * own, ny // 2
    rows = half // CHUNKS
    exchanges = 2 * ITERS
    me = lax.axis_index("gz")
    q = me % 4
    base = me - q
    h, s = q // 2, q % 2
    lower, upper = me - 3 + 2 * s, me + 1 + 2 * s
    mate = me + 2 - 4 * h
    has_lo = lower >= 0
    has_hi = upper < n
    partners = []
    for r in range(rounds):
        bit = 1 << r
        partners.append(me + bit * (1 - 2 * ((me // bit) % 2)))
    sums = [partners[0]] + partners[2:]
    free = s == h

    hbm = (init_hbm, coef_hbm, obs_hbm, wgt_hbm)
    held = (None, coef, obs, wgt)
    for array in range(2):
        src = hbm[array].at[:, pl.ds(pl.multiple_of(half - h * rows, PAD), rows), :]
        pltpu.make_async_copy(src, first.at[array], first_sem).start()

    barrier = pltpu.get_barrier_semaphore()

    def greet(device):
        pl.semaphore_signal(barrier, inc=1, device_id=(device,), device_id_type=MESH)

    for i in range(1, 4):
        greet(base + (q + i) % 4)
    outside_lo = (s == 0) & has_lo
    outside_hi = (s == 1) & has_hi

    @pl.when(outside_lo)
    def _():
        greet(lower)

    @pl.when(outside_hi)
    def _():
        greet(upper)

    zero_rows = jnp.zeros((PAD, nx), jnp.float32)
    outer = pl.multiple_of(h * (PAD + half), PAD)
    inner = pl.multiple_of((1 - h) * (PAD + half), PAD)

    crossing = outside_lo | outside_hi

    @pl.when(crossing)
    def _():
        pl.semaphore_wait(barrier, 4)

    @pl.when(jnp.logical_not(crossing))
    def _():
        pl.semaphore_wait(barrier, 3)

    def place(side_half, j):
        return j if side_half == 1 else CHUNKS - 1 - j

    def feed(array, j):
        for to in range(2):
            dest = base + 2 * to + q // 2
            row = place(to, j) * rows
            slot = pl.ds(s * own, own)
            if array == 0:
                src = init_hbm.at[:, pl.ds(pl.multiple_of(to * half + row, PAD), rows), :]
                dst = st.at[0, slot, pl.ds(pl.multiple_of(PAD + row, PAD), rows), :]
            else:
                src = hbm[array].at[:, pl.ds(pl.multiple_of(to * half + row, PAD), rows), :]
                dst = held[array].at[slot, pl.ds(pl.multiple_of(row, PAD), rows), :]
            arrived = in_recv.at[array // 2, j]
            distant = dest != me
            if isinstance(j, int) and j == 0:
                across_chips = q // 2 != to
                distant = distant & (q // 2 == to)

                @pl.when(across_chips)
                def _():
                    pltpu.make_async_remote_copy(
                        src_ref=first.at[array], dst_ref=dst, send_sem=in_send.at[to], recv_sem=arrived,
                        device_id=(dest,), device_id_type=MESH,
                    ).start()

            @pl.when(dest == me)
            def _():
                pltpu.make_async_copy(src, dst, arrived).start()

            @pl.when(distant)
            def _():
                pltpu.make_async_remote_copy(
                    src_ref=src, dst_ref=dst, send_sem=in_send.at[to], recv_sem=arrived,
                    device_id=(dest,), device_id_type=MESH,
                ).start()

    def await_copy(ref, sem):
        pltpu.make_async_copy(ref, ref, sem).wait()

    def fed(kind, j):
        await_copy(st.at[pl.ds(0, 2), :, pl.ds(0, rows), :], in_recv.at[kind, j])

    await_copy(first, first_sem)
    for j in range(3):
        feed(0, j)
        feed(1, j)

    def clear_pad(e, carry):
        for p in range(planes):
            st[e, p, pl.ds(outer, PAD), :] = zero_rows
        return carry

    lax.fori_loop(0, exchanges, clear_pad, 0)

    def clear_halo(side):
        def clear(i, carry):
            e = i // (half // PAD)
            row = pl.multiple_of((i % (half // PAD)) * PAD, PAD)
            halo[side, e, pl.ds(row, PAD), :] = zero_rows
            return carry

        lax.fori_loop(0, exchanges * (half // PAD), clear, 0)

    @pl.when(jnp.logical_not(has_lo))
    def _():
        clear_halo(0)

    @pl.when(jnp.logical_not(has_hi))
    def _():
        clear_halo(1)

    acc[...] = jnp.zeros_like(acc)
    def send(e, at, j):
        here = pl.ds(at, rows)
        padded = pl.ds(pl.multiple_of(PAD + at, PAD), rows)

        def copy(side, device):
            pltpu.make_async_remote_copy(
                src_ref=st.at[e, (planes - 1) * (1 - side), padded, :],
                dst_ref=halo.at[side, e, here, :],
                send_sem=halo_send.at[side], recv_sem=halo_recv.at[e, j % RING],
                device_id=(device,), device_id_type=MESH,
            ).start()

        @pl.when(has_hi)
        def _():
            copy(0, upper)

        @pl.when(has_lo)
        def _():
            copy(1, lower)

    def receive(e, at, j):
        here = pl.ds(at, rows)
        arrived = halo_recv.at[e, j % RING]

        @pl.when(has_lo & has_hi)
        def _():
            await_copy(halo.at[:, e, here, :], arrived)

        @pl.when(jnp.logical_not(has_lo & has_hi))
        def _():
            await_copy(halo.at[0, e, here, :], arrived)

    def edge_copy(e):
        return pltpu.make_async_remote_copy(
            src_ref=edge_out.at[e], dst_ref=edge_in.at[e],
            send_sem=edge_send, recv_sem=edge_recv.at[e % 2],
            device_id=(mate,), device_id_type=MESH,
        )

    def stage_edge(e):
        at = pl.multiple_of(PAD + (1 - h) * (half - PAD), PAD)
        for p in range(planes):
            block = st[e, p, pl.ds(at, PAD), :]
            edge_out[e, p:p + 1, :] = jnp.where(h == 0, block[PAD - 1:PAD], block[0:1])

    def take_edge(e):
        edge_copy(e).wait_recv()
        for p in range(planes):
            st[e, p, pl.ds(inner, PAD), :] = jnp.broadcast_to(edge_in[e, p:p + 1, :], (PAD, nx))

    lane = lax.broadcasted_iota(jnp.int32, (TILE, nx), 1)
    leftmost = lane == 0
    rightmost = lane == nx - 1

    def laplace(e, p, row):
        here = pl.ds(row, TILE)
        padded = pl.ds(pl.multiple_of(row + PAD, PAD), TILE)
        tall = st[e, p, pl.ds(row, TILE + 2 * PAD), :]
        mid = tall[PAD:PAD + TILE]
        beside = tall[PAD + 1:PAD + 1 + TILE] + tall[PAD - 1:PAD - 1 + TILE]
        beside = beside + jnp.where(rightmost, 0.0, pltpu.roll(mid, nx - 1, 1))
        beside = beside + jnp.where(leftmost, 0.0, pltpu.roll(mid, 1, 1))
        above = st[e, p + 1, padded, :] if p + 1 < planes else halo[1, e, here, :]
        below = st[e, p - 1, padded, :] if p > 0 else halo[0, e, here, :]
        return mid, beside + above + below - 6.0 * mid

    def ship(which, source, target, m):
        at = pl.multiple_of((CHUNKS - 2 - 2 * m) * (1 - h) * rows + 2 * m * h * rows, PAD)
        for o in range(2):
            dest = base + 2 * s + o
            src = source.at[pl.ds(o * own, own), pl.ds(at, 2 * rows), :]
            dst = target.at[:, pl.ds(pl.multiple_of(h * half + at, PAD), 2 * rows), :]

            @pl.when(dest == me)
            def _():
                pltpu.make_async_copy(src, dst, out_recv).start()

            @pl.when(dest != me)
            def _():
                pltpu.make_async_remote_copy(
                    src_ref=src, dst_ref=dst, send_sem=out_send.at[o],
                    recv_sem=out_recv, device_id=(dest,), device_id_type=MESH,
                ).start()

    def stage(e, j):
        at = pl.multiple_of((CHUNKS - 1 - j) * (1 - h) * rows + j * h * rows, PAD)
        @pl.when(j == 0)
        def _():
            take_edge(e)

        if e == ITERS - 1:
            fed(1, j)
        receive(e, at, j)

        def tile(t, carry):
            row = pl.multiple_of(at + t * TILE, TILE)
            here = pl.ds(row, TILE)
            padded = pl.ds(pl.multiple_of(row + PAD, PAD), TILE)
            for p in range(planes):
                mid, slope = laplace(e, p, row)
                if e < ITERS - 1:
                    sl[e, p, here, :] = slope
                    st[e + 1, p, padded, :] = mid + time_step * coef[p, here, :] * slope
                elif e == ITERS - 1:
                    c = coef[p, here, :]
                    resid = mid + time_step * c * slope - obs[p, here, :]
                    weighted = wgt[p, here, :] * resid
                    acc[...] += weighted * resid
                    aacc[p, here, :] = weighted
                    gacc[p, here, :] = time_step * weighted * slope
                    st[e + 1, p, padded, :] = c * weighted
                else:
                    lam = aacc[p, here, :] + time_step * slope
                    aacc[p, here, :] = lam
                    if e < exchanges - 1:
                        gacc[p, here, :] += time_step * lam * sl[exchanges - 2 - e, p, here, :]
                        st[e + 1, p, padded, :] = coef[p, here, :] * lam
            return carry

        lax.fori_loop(0, rows // TILE, tile, 0)
        if e < exchanges - 1:
            @pl.when(j == 0)
            def _():
                stage_edge(e + 1)

            send(e + 1, at, j)

            @pl.when(j == 0)
            def _():
                edge_copy(e + 1).start()

    def exchange(r):
        return pltpu.make_async_remote_copy(
            src_ref=part.at[2 * r], dst_ref=part.at[2 * r + 1],
            send_sem=psend_sem, recv_sem=precv_sem.at[r],
            device_id=(sums[r],), device_id_type=MESH,
        )

    def across(o):
        return pltpu.make_async_remote_copy(
            src_ref=part.at[2 * rounds - 2], dst_ref=part.at[2 * rounds - 1],
            send_sem=psend_sem, recv_sem=precv_sem.at[rounds - 1],
            device_id=(base + 2 * (1 - h) + o,), device_id_type=MESH,
        )

    def total_round(r):
        if r == 0:
            whole = acc[...]
            narrow = whole[:, 0:128]
            for i in range(1, nx // 128):
                narrow = narrow + whole[:, 128 * i:128 * i + 128]
            part[0] = narrow
        else:
            exchange(r - 1).wait_recv()
            part[2 * r] = part[2 * r - 2] + part[2 * r - 1]
        if r < rounds - 1:
            exchange(r).start()
        else:
            @pl.when(free)
            def _():
                across(0).start()
                across(1).start()

    summed = CHUNKS + ITERS - 1
    ticks = CHUNKS + exchanges

    def tick(t, carry):
        @pl.when(t < CHUNKS)
        def _():
            at = pl.multiple_of((CHUNKS - 1 - t) * (1 - h) * rows + t * h * rows, PAD)
            fed(0, t)

            @pl.when(t == 0)
            def _():
                stage_edge(0)
                edge_copy(0).start()

            send(0, at, t)

        for e in range(exchanges):
            j = t - 1 - e

            @pl.when((j >= 0) & (j < CHUNKS))
            def _():
                stage(e, j)

        @pl.when(t + 3 < CHUNKS)
        def _():
            feed(0, t + 3)
            feed(1, t + 3)

        late = t + 2 - ITERS + 1

        @pl.when((late >= 0) & (late < CHUNKS))
        def _():
            feed(2, late)
            feed(3, late)

        for which, source, target, begin in ((0, gacc, grad_out, CHUNKS - 2), (1, aacc, adj_out, CHUNKS - 1)):
            m, final = t - begin, CHUNKS // 2 - 1

            @pl.when((m >= 0) & (m < final))
            def _():
                ship(which, source, target, m)

            @pl.when(m == final + 1)
            def _():
                ship(which, source, target, final)

        for r in range(min(rounds, ticks - summed)):
            @pl.when(t == summed + r)
            def _():
                total_round(r)

        return carry

    lax.fori_loop(0, ticks, tick, 0)
    for r in range(ticks - summed, rounds):
        total_round(r)

    across(0).wait_recv()
    whole = part[2 * rounds - 2] + part[2 * rounds - 1]
    whole = jnp.sum(jnp.sum(whole, axis=1, keepdims=True), axis=0, keepdims=True)
    misfit_out[...] = jnp.sqrt(jnp.broadcast_to(whole, (8, 128)) / cells + 1e-06)

    slabs = st.at[pl.ds(0, 2), :, pl.ds(0, half), :]
    await_copy(slabs, out_recv)
    for o in range(2):
        @pl.when(base + 2 * s + o != me)
        def _():
            await_copy(coef, out_send.at[o])
    for to in range(2):
        @pl.when(base + 2 * to + q // 2 != me)
        def _():
            await_copy(slabs, in_send.at[to])

    @pl.when(has_hi)
    def _():
        await_copy(halo.at[0], halo_send.at[0])

    @pl.when(has_lo)
    def _():
        await_copy(halo.at[1], halo_send.at[1])

    await_copy(edge_out, edge_send)

    @pl.when(free)
    def _():
        await_copy(part.at[pl.ds(0, rounds + 1)], psend_sem)

    @pl.when(jnp.logical_not(free))
    def _():
        await_copy(part.at[pl.ds(0, rounds - 1)], psend_sem)


def finish(grad, adj, misfit, grad_out, adj_out, misfit_out, scaled, sem):
    own, ny, nx = grad.shape
    scale = misfit[...]
    misfit_out[...] = scale[0:1, 0:1]
    inverse = 1.0 / scale
    wide = jnp.concatenate([inverse] * (nx // 128), axis=1)
    for which, (source, target) in enumerate(((grad, grad_out), (adj, adj_out))):
        for p in range(own):
            def piece(i, carry):
                at = pl.multiple_of(i * PIECE, PIECE)
                for r in range(PIECE // TILE):
                    row = pl.multiple_of(at + r * TILE, TILE)
                    scaled[which, p, pl.ds(row, TILE), :] = source[p, pl.ds(row, TILE), :] * wide
                here = pl.ds(at, PIECE)
                pltpu.make_async_copy(scaled.at[which, p, here, :], target.at[p, here, :], sem).start()
                return carry

            lax.fori_loop(0, ny // PIECE, piece, 0)
    pltpu.make_async_copy(scaled, scaled, sem).wait()


def solution(mesh):
    n = mesh.shape["gz"]
    rounds = n.bit_length() - 1

    def on_device(coefficient, initial_field, observed, misfit_weight):
        own, ny, nx = coefficient.shape
        planes, half = 2 * own, ny // 2
        slab = jax.ShapeDtypeStruct(coefficient.shape, jnp.float32)
        exchanges = 2 * ITERS
        block = pltpu.VMEM((planes, half, nx), jnp.float32)
        edge = pltpu.VMEM((exchanges, planes, nx), jnp.float32)
        dma = pltpu.SemaphoreType.DMA
        grad, adj, misfit = pl.pallas_call(
            functools.partial(kernel, n, rounds, float(n * own * ny * nx)),
            out_shape=(slab, slab, jax.ShapeDtypeStruct((8, 128), jnp.float32)),
            in_specs=[pl.BlockSpec(memory_space=pl.ANY)] * 4,
            out_specs=[pl.BlockSpec(memory_space=pl.ANY)] * 2 + [pl.BlockSpec(memory_space=pltpu.VMEM)],
            scratch_shapes=[
                pltpu.VMEM((exchanges, planes, half + 2 * PAD, nx), jnp.float32),
                pltpu.VMEM((ITERS - 1, planes, half, nx), jnp.float32),
                pltpu.VMEM((2, exchanges, half, nx), jnp.float32),
                block, block, block, block, block,
                pltpu.VMEM((TILE, nx), jnp.float32),
                pltpu.VMEM((2 * rounds, 8, 128), jnp.float32),
                edge, edge,
                dma((2,)), dma((2, CHUNKS)),
                dma((2,)), dma((exchanges, RING)),
                dma, dma((2,)),
                dma((2,)), dma,
                dma, dma((rounds,)),
                pltpu.VMEM((2, own, half // CHUNKS, nx), jnp.float32), dma,
            ],
            compiler_params=pltpu.CompilerParams(
                collective_id=0, has_side_effects=True, vmem_limit_bytes=48 * 1024 * 1024
            ),
        )(coefficient, initial_field, observed, misfit_weight)
        vmem = pl.BlockSpec(memory_space=pltpu.VMEM)
        grad, adj, misfit = pl.pallas_call(
            finish,
            out_shape=(slab, slab, jax.ShapeDtypeStruct((1, 1), jnp.float32)),
            in_specs=[vmem] * 3,
            out_specs=[pl.BlockSpec(memory_space=pltpu.HBM)] * 2 + [vmem],
            scratch_shapes=[pltpu.VMEM((2, *coefficient.shape), jnp.float32), dma],
            compiler_params=pltpu.CompilerParams(vmem_limit_bytes=6 * 1024 * 1024),
        )(grad, adj, misfit)
        return grad, adj, misfit.reshape(())

    placed = P("gz", None, None)
    return jax.shard_map(
        on_device,
        mesh=mesh,
        in_specs=(placed,) * 4,
        out_specs=(placed, placed, P()),
        check_vma=False,
    )
```

```python
import functools

import jax
import jax.numpy as jnp
from jax import lax
from jax.experimental import pallas as pl
from jax.experimental.pallas import tpu as pltpu
from jax.sharding import PartitionSpec as P

ITERS = 4
time_step = 0.125
MESH = pl.DeviceIdType.MESH
PAD = 8
TILE = 8
CHUNKS = 16
RING = 4
PIECE = 128
SHIP = 12


def kernel(n, rounds, cells, coef_hbm, init_hbm, obs_hbm, wgt_hbm, grad_out, adj_out, misfit_out,
           st, sl, halo, coef, obs, wgt, gacc, aacc, acc, part, edge_out, edge_in,
           in_send, in_recv, halo_send, halo_recv, edge_send, edge_recv,
           out_send, out_recv, psend_sem, precv_sem, first, first_sem):
    own, ny, nx = coef_hbm.shape
    planes, half = 2 * own, ny // 2
    rows = half // CHUNKS
    exchanges = 2 * ITERS
    me = lax.axis_index("gz")
    q = me % 4
    base = me - q
    h, s = q // 2, q % 2
    lower, upper = me - 3 + 2 * s, me + 1 + 2 * s
    mate = me + 2 - 4 * h
    has_lo = lower >= 0
    has_hi = upper < n
    partners = []
    for r in range(rounds):
        bit = 1 << r
        partners.append(me + bit * (1 - 2 * ((me // bit) % 2)))
    sums = [partners[0]] + partners[2:]
    free = s == h

    hbm = (init_hbm, coef_hbm, obs_hbm, wgt_hbm)
    held = (None, coef, obs, wgt)
    for array in range(2):
        src = hbm[array].at[:, pl.ds(pl.multiple_of(half - h * rows, PAD), rows), :]
        pltpu.make_async_copy(src, first.at[array], first_sem).start()

    barrier = pltpu.get_barrier_semaphore()

    def greet(device):
        pl.semaphore_signal(barrier, inc=1, device_id=(device,), device_id_type=MESH)

    below, beyond = base > 0, base + 4 < n
    middle = (q == 1) | (q == 2)
    greet(base + jnp.where(middle, 3 - q, 1 + q // 3))

    @pl.when(middle)
    def _():
        greet(base + jnp.where(q == 1, 3, 0))

    @pl.when((h == s) & jnp.where(h == 0, below, beyond))
    def _():
        greet(me - 3 + 6 * h)

    @pl.when(middle & jnp.where(h == 0, beyond, below))
    def _():
        greet(me + 4 - 8 * h)

    zero_rows = jnp.zeros((PAD, nx), jnp.float32)
    outer = pl.multiple_of(h * (PAD + half), PAD)
    inner = pl.multiple_of((1 - h) * (PAD + half), PAD)

    for central in (False, True):
        for sides in range(3 if central else 1):
            count = below.astype(jnp.int32) + beyond.astype(jnp.int32)

            @pl.when(middle & (count == sides) if central else jnp.logical_not(middle))
            def _():
                pl.semaphore_wait(barrier, 2 + sides if central else 1)

    def place(side_half, j):
        return j if side_half == 1 else CHUNKS - 1 - j

    def feed(array, j):
        for to in range(2):
            dest = base + 2 * to + q // 2
            row = place(to, j) * rows
            slot = pl.ds(s * own, own)
            if array == 0:
                src = init_hbm.at[:, pl.ds(pl.multiple_of(to * half + row, PAD), rows), :]
                dst = st.at[0, slot, pl.ds(pl.multiple_of(PAD + row, PAD), rows), :]
            else:
                src = hbm[array].at[:, pl.ds(pl.multiple_of(to * half + row, PAD), rows), :]
                dst = held[array].at[slot, pl.ds(pl.multiple_of(row, PAD), rows), :]
            arrived = in_recv.at[array // 2, j]
            distant = dest != me
            if isinstance(j, int) and j == 0:
                across_chips = q // 2 != to
                distant = distant & (q // 2 == to)

                @pl.when(across_chips)
                def _():
                    pltpu.make_async_remote_copy(
                        src_ref=first.at[array], dst_ref=dst, send_sem=in_send.at[to], recv_sem=arrived,
                        device_id=(dest,), device_id_type=MESH,
                    ).start()

            @pl.when(dest == me)
            def _():
                pltpu.make_async_copy(src, dst, arrived).start()

            @pl.when(distant)
            def _():
                pltpu.make_async_remote_copy(
                    src_ref=src, dst_ref=dst, send_sem=in_send.at[to], recv_sem=arrived,
                    device_id=(dest,), device_id_type=MESH,
                ).start()

    def await_copy(ref, sem):
        pltpu.make_async_copy(ref, ref, sem).wait()

    def fed(kind, j):
        await_copy(st.at[pl.ds(0, 2), :, pl.ds(0, rows), :], in_recv.at[kind, j])

    await_copy(first, first_sem)
    for j in range(3):
        feed(0, j)
        feed(1, j)

    def clear_pad(e, carry):
        for p in range(planes):
            st[e, p, pl.ds(outer, PAD), :] = zero_rows
        return carry

    lax.fori_loop(0, exchanges, clear_pad, 0)

    def clear_halo(side):
        def clear(i, carry):
            e = i // (half // PAD)
            row = pl.multiple_of((i % (half // PAD)) * PAD, PAD)
            halo[side, e, pl.ds(row, PAD), :] = zero_rows
            return carry

        lax.fori_loop(0, exchanges * (half // PAD), clear, 0)

    @pl.when(jnp.logical_not(has_lo))
    def _():
        clear_halo(0)

    @pl.when(jnp.logical_not(has_hi))
    def _():
        clear_halo(1)

    acc[...] = jnp.zeros_like(acc)
    def send(e, at, j):
        here = pl.ds(at, rows)
        padded = pl.ds(pl.multiple_of(PAD + at, PAD), rows)

        def copy(side, device):
            pltpu.make_async_remote_copy(
                src_ref=st.at[e, (planes - 1) * (1 - side), padded, :],
                dst_ref=halo.at[side, e, here, :],
                send_sem=halo_send.at[side], recv_sem=halo_recv.at[e, j % RING],
                device_id=(device,), device_id_type=MESH,
            ).start()

        @pl.when(has_hi)
        def _():
            copy(0, upper)

        @pl.when(has_lo)
        def _():
            copy(1, lower)

    def receive(e, at, j):
        here = pl.ds(at, rows)
        arrived = halo_recv.at[e, j % RING]

        @pl.when(has_lo & has_hi)
        def _():
            await_copy(halo.at[:, e, here, :], arrived)

        @pl.when(jnp.logical_not(has_lo & has_hi))
        def _():
            await_copy(halo.at[0, e, here, :], arrived)

    def edge_copy(e):
        return pltpu.make_async_remote_copy(
            src_ref=edge_out.at[e], dst_ref=edge_in.at[e],
            send_sem=edge_send, recv_sem=edge_recv.at[e % 2],
            device_id=(mate,), device_id_type=MESH,
        )

    def stage_edge(e):
        at = pl.multiple_of(PAD + (1 - h) * (half - PAD), PAD)
        for p in range(planes):
            block = st[e, p, pl.ds(at, PAD), :]
            edge_out[e, p:p + 1, :] = jnp.where(h == 0, block[PAD - 1:PAD], block[0:1])

    def take_edge(e):
        edge_copy(e).wait_recv()
        for p in range(planes):
            st[e, p, pl.ds(inner, PAD), :] = jnp.broadcast_to(edge_in[e, p:p + 1, :], (PAD, nx))

    lane = lax.broadcasted_iota(jnp.int32, (TILE, nx), 1)
    leftmost = lane == 0
    rightmost = lane == nx - 1

    def laplace(e, p, row):
        here = pl.ds(row, TILE)
        padded = pl.ds(pl.multiple_of(row + PAD, PAD), TILE)
        tall = st[e, p, pl.ds(row, TILE + 2 * PAD), :]
        mid = tall[PAD:PAD + TILE]
        beside = tall[PAD + 1:PAD + 1 + TILE] + tall[PAD - 1:PAD - 1 + TILE]
        beside = beside + jnp.where(rightmost, 0.0, pltpu.roll(mid, nx - 1, 1))
        beside = beside + jnp.where(leftmost, 0.0, pltpu.roll(mid, 1, 1))
        above = st[e, p + 1, padded, :] if p + 1 < planes else halo[1, e, here, :]
        below = st[e, p - 1, padded, :] if p > 0 else halo[0, e, here, :]
        return mid, beside + above + below - 6.0 * mid

    def ship(which, source, target, m):
        at = pl.multiple_of((CHUNKS - 2 - 2 * m) * (1 - h) * rows + 2 * m * h * rows, PAD)
        for o in range(2):
            dest = base + 2 * s + o
            src = source.at[pl.ds(o * own, own), pl.ds(at, 2 * rows), :]
            dst = target.at[:, pl.ds(pl.multiple_of(h * half + at, PAD), 2 * rows), :]

            @pl.when(dest == me)
            def _():
                pltpu.make_async_copy(src, dst, out_recv).start()

            @pl.when(dest != me)
            def _():
                pltpu.make_async_remote_copy(
                    src_ref=src, dst_ref=dst, send_sem=out_send.at[o],
                    recv_sem=out_recv, device_id=(dest,), device_id_type=MESH,
                ).start()

    def stage(e, j):
        at = pl.multiple_of((CHUNKS - 1 - j) * (1 - h) * rows + j * h * rows, PAD)
        @pl.when(j == 0)
        def _():
            take_edge(e)

        if e == ITERS - 1:
            fed(1, j)
        receive(e, at, j)

        def tile(t, carry):
            row = pl.multiple_of(at + t * TILE, TILE)
            here = pl.ds(row, TILE)
            padded = pl.ds(pl.multiple_of(row + PAD, PAD), TILE)
            for p in range(planes):
                mid, slope = laplace(e, p, row)
                if e < ITERS - 1:
                    sl[e, p, here, :] = slope
                    st[e + 1, p, padded, :] = mid + time_step * coef[p, here, :] * slope
                elif e == ITERS - 1:
                    c = coef[p, here, :]
                    resid = mid + time_step * c * slope - obs[p, here, :]
                    weighted = wgt[p, here, :] * resid
                    acc[...] += weighted * resid
                    aacc[p, here, :] = weighted
                    gacc[p, here, :] = time_step * weighted * slope
                    st[e + 1, p, padded, :] = c * weighted
                else:
                    lam = aacc[p, here, :] + time_step * slope
                    aacc[p, here, :] = lam
                    if e < exchanges - 1:
                        gacc[p, here, :] += time_step * lam * sl[exchanges - 2 - e, p, here, :]
                        st[e + 1, p, padded, :] = coef[p, here, :] * lam
            return carry

        lax.fori_loop(0, rows // TILE, tile, 0)
        if e < exchanges - 1:
            @pl.when(j == 0)
            def _():
                stage_edge(e + 1)

            send(e + 1, at, j)

            @pl.when(j == 0)
            def _():
                edge_copy(e + 1).start()

    def exchange(r):
        return pltpu.make_async_remote_copy(
            src_ref=part.at[2 * r], dst_ref=part.at[2 * r + 1],
            send_sem=psend_sem, recv_sem=precv_sem.at[r],
            device_id=(sums[r],), device_id_type=MESH,
        )

    def across(o):
        return pltpu.make_async_remote_copy(
            src_ref=part.at[2 * rounds - 2], dst_ref=part.at[2 * rounds - 1],
            send_sem=psend_sem, recv_sem=precv_sem.at[rounds - 1],
            device_id=(base + 2 * (1 - h) + o,), device_id_type=MESH,
        )

    def total_round(r):
        if r == 0:
            whole = acc[...]
            narrow = whole[:, 0:128]
            for i in range(1, nx // 128):
                narrow = narrow + whole[:, 128 * i:128 * i + 128]
            part[0] = narrow
        else:
            exchange(r - 1).wait_recv()
            part[2 * r] = part[2 * r - 2] + part[2 * r - 1]
        if r < rounds - 1:
            exchange(r).start()
        else:
            @pl.when(free)
            def _():
                across(0).start()
                across(1).start()

    summed = CHUNKS + ITERS - 1
    ticks = CHUNKS + exchanges

    def tick(t, carry):
        @pl.when(t < CHUNKS)
        def _():
            at = pl.multiple_of((CHUNKS - 1 - t) * (1 - h) * rows + t * h * rows, PAD)
            fed(0, t)

            @pl.when(t == 0)
            def _():
                stage_edge(0)
                edge_copy(0).start()

            send(0, at, t)

        for e in range(exchanges):
            j = t - 1 - e

            @pl.when((j >= 0) & (j < CHUNKS))
            def _():
                stage(e, j)

        @pl.when(t + 3 < CHUNKS)
        def _():
            feed(0, t + 3)
            feed(1, t + 3)

        late = t + 2 - ITERS + 1

        @pl.when((late >= 0) & (late < CHUNKS))
        def _():
            feed(2, late)
            feed(3, late)

        for which, source, target in ((0, gacc, grad_out), (1, aacc, adj_out)):
            early, since = t - SHIP - which, t - exchanges - which

            @pl.when((early >= 0) & (early <= SHIP - exchanges) & (early < CHUNKS // 2))
            def _():
                ship(which, source, target, early)

            @pl.when((since % 2 == 0) & (since // 2 > SHIP - exchanges) & (since // 2 < CHUNKS // 2))
            def _():
                ship(which, source, target, since // 2)

        for r in range(min(rounds, ticks - summed)):
            @pl.when(t == summed + r)
            def _():
                total_round(r)

        return carry

    lax.fori_loop(0, ticks, tick, 0)
    for r in range(ticks - summed, rounds):
        total_round(r)

    across(0).wait_recv()
    whole = part[2 * rounds - 2] + part[2 * rounds - 1]
    whole = jnp.sum(jnp.sum(whole, axis=1, keepdims=True), axis=0, keepdims=True)
    misfit_out[...] = jnp.sqrt(jnp.broadcast_to(whole, (8, 128)) / cells + 1e-06)

    slabs = st.at[pl.ds(0, 2), :, pl.ds(0, half), :]
    await_copy(slabs, out_recv)
    for o in range(2):
        @pl.when(base + 2 * s + o != me)
        def _():
            await_copy(coef, out_send.at[o])
    for to in range(2):
        @pl.when(base + 2 * to + q // 2 != me)
        def _():
            await_copy(slabs, in_send.at[to])

    @pl.when(has_hi)
    def _():
        await_copy(halo.at[0], halo_send.at[0])

    @pl.when(has_lo)
    def _():
        await_copy(halo.at[1], halo_send.at[1])

    await_copy(edge_out, edge_send)

    @pl.when(free)
    def _():
        await_copy(part.at[pl.ds(0, rounds + 1)], psend_sem)

    @pl.when(jnp.logical_not(free))
    def _():
        await_copy(part.at[pl.ds(0, rounds - 1)], psend_sem)


def finish(grad, adj, misfit, grad_out, adj_out, misfit_out, scaled, sem):
    own, ny, nx = grad.shape
    scale = misfit[...]
    misfit_out[...] = scale[0:1, 0:1]
    inverse = 1.0 / scale
    wide = jnp.concatenate([inverse] * (nx // 128), axis=1)
    for which, (source, target) in enumerate(((grad, grad_out), (adj, adj_out))):
        for p in range(own):
            def piece(i, carry):
                at = pl.multiple_of(i * PIECE, PIECE)
                for r in range(PIECE // TILE):
                    row = pl.multiple_of(at + r * TILE, TILE)
                    scaled[which, p, pl.ds(row, TILE), :] = source[p, pl.ds(row, TILE), :] * wide
                here = pl.ds(at, PIECE)
                pltpu.make_async_copy(scaled.at[which, p, here, :], target.at[p, here, :], sem).start()
                return carry

            lax.fori_loop(0, ny // PIECE, piece, 0)
    pltpu.make_async_copy(scaled, scaled, sem).wait()


def solution(mesh):
    n = mesh.shape["gz"]
    rounds = n.bit_length() - 1

    def on_device(coefficient, initial_field, observed, misfit_weight):
        own, ny, nx = coefficient.shape
        planes, half = 2 * own, ny // 2
        slab = jax.ShapeDtypeStruct(coefficient.shape, jnp.float32)
        exchanges = 2 * ITERS
        block = pltpu.VMEM((planes, half, nx), jnp.float32)
        edge = pltpu.VMEM((exchanges, planes, nx), jnp.float32)
        dma = pltpu.SemaphoreType.DMA
        grad, adj, misfit = pl.pallas_call(
            functools.partial(kernel, n, rounds, float(n * own * ny * nx)),
            out_shape=(slab, slab, jax.ShapeDtypeStruct((8, 128), jnp.float32)),
            in_specs=[pl.BlockSpec(memory_space=pl.ANY)] * 4,
            out_specs=[pl.BlockSpec(memory_space=pl.ANY)] * 2 + [pl.BlockSpec(memory_space=pltpu.VMEM)],
            scratch_shapes=[
                pltpu.VMEM((exchanges, planes, half + 2 * PAD, nx), jnp.float32),
                pltpu.VMEM((ITERS - 1, planes, half, nx), jnp.float32),
                pltpu.VMEM((2, exchanges, half, nx), jnp.float32),
                block, block, block, block, block,
                pltpu.VMEM((TILE, nx), jnp.float32),
                pltpu.VMEM((2 * rounds, 8, 128), jnp.float32),
                edge, edge,
                dma((2,)), dma((2, CHUNKS)),
                dma((2,)), dma((exchanges, RING)),
                dma, dma((2,)),
                dma((2,)), dma,
                dma, dma((rounds,)),
                pltpu.VMEM((2, own, half // CHUNKS, nx), jnp.float32), dma,
            ],
            compiler_params=pltpu.CompilerParams(
                collective_id=0, has_side_effects=True, vmem_limit_bytes=48 * 1024 * 1024
            ),
        )(coefficient, initial_field, observed, misfit_weight)
        vmem = pl.BlockSpec(memory_space=pltpu.VMEM)
        grad, adj, misfit = pl.pallas_call(
            finish,
            out_shape=(slab, slab, jax.ShapeDtypeStruct((1, 1), jnp.float32)),
            in_specs=[vmem] * 3,
            out_specs=[pl.BlockSpec(memory_space=pltpu.HBM)] * 2 + [vmem],
            scratch_shapes=[pltpu.VMEM((2, *coefficient.shape), jnp.float32), dma],
            compiler_params=pltpu.CompilerParams(vmem_limit_bytes=6 * 1024 * 1024),
        )(grad, adj, misfit)
        return grad, adj, misfit.reshape(())

    placed = P("gz", None, None)
    return jax.shard_map(
        on_device,
        mesh=mesh,
        in_specs=(placed,) * 4,
        out_specs=(placed, placed, P()),
        check_vma=False,
    )
```

```python
import functools

import jax
import jax.numpy as jnp
from jax import lax
from jax.experimental import pallas as pl
from jax.experimental.pallas import tpu as pltpu
from jax.sharding import PartitionSpec as P

ITERS = 4
time_step = 0.125
MESH = pl.DeviceIdType.MESH
PAD = 8
TILE = 8
CHUNKS = 16
RING = 4
GROUP = 4
SLOTS = 8
PIECE = 128
SHIP = 12


def kernel(n, rounds, cells, coef_hbm, init_hbm, obs_hbm, wgt_hbm, grad_out, adj_out, misfit_out,
           st, sl, halo, coef, obs, wgt, gacc, aacc, acc, part, edge_out, edge_in,
           in_send, in_recv, halo_send, halo_recv, edge_send, edge_recv,
           out_send, out_recv, psend_sem, precv_sem, first, first_sem):
    own, ny, nx = coef_hbm.shape
    planes, half = 2 * own, ny // 2
    rows = half // CHUNKS
    exchanges = 2 * ITERS
    me = lax.axis_index("gz")
    q = me % 4
    base = me - q
    h, s = q // 2, q % 2
    lower, upper = me - 3 + 2 * s, me + 1 + 2 * s
    mate = me + 2 - 4 * h
    has_lo = lower >= 0
    has_hi = upper < n
    partners = []
    for r in range(rounds):
        bit = 1 << r
        partners.append(me + bit * (1 - 2 * ((me // bit) % 2)))
    sums = [partners[0]] + partners[2:]
    free = s == h

    hbm = (init_hbm, coef_hbm, obs_hbm, wgt_hbm)
    held = (None, coef, obs, wgt)
    barrier = pltpu.get_barrier_semaphore()

    def greet(device):
        pl.semaphore_signal(barrier, inc=1, device_id=(device,), device_id_type=MESH)

    below, beyond = base > 0, base + 4 < n
    middle = (q == 1) | (q == 2)

    @pl.when(middle)
    def _():
        greet(base + jnp.where(q == 1, 3, 0))

    greet(base + jnp.where(middle, 3 - q, 1 + q // 3))

    @pl.when((h == s) & jnp.where(h == 0, below, beyond))
    def _():
        greet(me - 3 + 6 * h)

    @pl.when(middle & jnp.where(h == 0, beyond, below))
    def _():
        greet(me + 4 - 8 * h)

    for array in range(2):
        src = hbm[array].at[:, pl.ds(pl.multiple_of(half - h * rows, PAD), rows), :]
        pltpu.make_async_copy(src, first.at[array], first_sem).start()


    zero_rows = jnp.zeros((PAD, nx), jnp.float32)
    outer = pl.multiple_of(h * (PAD + half), PAD)
    inner = pl.multiple_of((1 - h) * (PAD + half), PAD)

    for central in (False, True):
        for sides in range(3 if central else 1):
            count = below.astype(jnp.int32) + beyond.astype(jnp.int32)

            @pl.when(middle & (count == sides) if central else jnp.logical_not(middle))
            def _():
                pl.semaphore_wait(barrier, 2 + sides if central else 1)

    def place(side_half, j):
        return j if side_half == 1 else CHUNKS - 1 - j

    def feed(array, j):
        for to in range(2):
            dest = base + 2 * to + q // 2
            row = place(to, j) * rows
            slot = pl.ds(s * own, own)
            if array == 0:
                src = init_hbm.at[:, pl.ds(pl.multiple_of(to * half + row, PAD), rows), :]
                dst = st.at[0, slot, pl.ds(pl.multiple_of(PAD + row, PAD), rows), :]
            else:
                src = hbm[array].at[:, pl.ds(pl.multiple_of(to * half + row, PAD), rows), :]
                dst = held[array].at[slot, pl.ds(pl.multiple_of(row, PAD), rows), :]
            arrived = in_recv.at[array // 2, j % SLOTS]
            distant = dest != me
            if isinstance(j, int) and j == 0:
                across_chips = q // 2 != to
                distant = distant & (q // 2 == to)

                @pl.when(across_chips)
                def _():
                    pltpu.make_async_remote_copy(
                        src_ref=first.at[array], dst_ref=dst, send_sem=in_send.at[to], recv_sem=arrived,
                        device_id=(dest,), device_id_type=MESH,
                    ).start()

            @pl.when(dest == me)
            def _():
                pltpu.make_async_copy(src, dst, arrived).start()

            @pl.when(distant)
            def _():
                pltpu.make_async_remote_copy(
                    src_ref=src, dst_ref=dst, send_sem=in_send.at[to], recv_sem=arrived,
                    device_id=(dest,), device_id_type=MESH,
                ).start()

    def await_copy(ref, sem):
        pltpu.make_async_copy(ref, ref, sem).wait()

    def fed(kind, j):
        await_copy(st.at[pl.ds(0, 2), :, pl.ds(0, rows), :], in_recv.at[kind, j % SLOTS])

    await_copy(first, first_sem)
    for j in range(3):
        feed(0, j)
        feed(1, j)

    def clear_pad(e, carry):
        for p in range(planes):
            st[e, p, pl.ds(outer, PAD), :] = zero_rows
        return carry

    lax.fori_loop(0, exchanges, clear_pad, 0)

    def clear_halo(side):
        def clear(i, carry):
            e = i // (half // PAD)
            row = pl.multiple_of((i % (half // PAD)) * PAD, PAD)
            halo[side, e, pl.ds(row, PAD), :] = zero_rows
            return carry

        lax.fori_loop(0, exchanges * (half // PAD), clear, 0)

    @pl.when(jnp.logical_not(has_lo))
    def _():
        clear_halo(0)

    @pl.when(jnp.logical_not(has_hi))
    def _():
        clear_halo(1)

    acc[...] = jnp.zeros_like(acc)
    def send(e, at, j):
        here = pl.ds(at, rows)
        padded = pl.ds(pl.multiple_of(PAD + at, PAD), rows)

        def copy(side, device):
            pltpu.make_async_remote_copy(
                src_ref=st.at[e, (planes - 1) * (1 - side), padded, :],
                dst_ref=halo.at[side, e, here, :],
                send_sem=halo_send.at[side], recv_sem=halo_recv.at[e // GROUP, (j + e + 1) % RING],
                device_id=(device,), device_id_type=MESH,
            ).start()

        @pl.when(has_hi)
        def _():
            copy(0, upper)

        @pl.when(has_lo)
        def _():
            copy(1, lower)

    def receive(group, t):
        first_stage = group * GROUP
        count = jnp.minimum(first_stage + GROUP, t) - jnp.maximum(first_stage, t - CHUNKS)
        arrived = halo_recv.at[group, t % RING]
        for stages in range(1, GROUP + 1):
            for sides in (1, 2):
                @pl.when((count == stages) & ((has_lo & has_hi) == (sides == 2)))
                def _():
                    await_copy(halo.at[pl.ds(0, sides), pl.ds(0, stages), pl.ds(0, rows), :], arrived)

    def edge_copy(e):
        return pltpu.make_async_remote_copy(
            src_ref=edge_out.at[e], dst_ref=edge_in.at[e],
            send_sem=edge_send, recv_sem=edge_recv.at[e % 2],
            device_id=(mate,), device_id_type=MESH,
        )

    def stage_edge(e):
        at = pl.multiple_of(PAD + (1 - h) * (half - PAD), PAD)
        for p in range(planes):
            block = st[e, p, pl.ds(at, PAD), :]
            edge_out[e, p:p + 1, :] = jnp.where(h == 0, block[PAD - 1:PAD], block[0:1])

    def take_edge(e):
        edge_copy(e).wait_recv()
        for p in range(planes):
            st[e, p, pl.ds(inner, PAD), :] = jnp.broadcast_to(edge_in[e, p:p + 1, :], (PAD, nx))

    lane = lax.broadcasted_iota(jnp.int32, (TILE, nx), 1)
    leftmost = lane == 0
    rightmost = lane == nx - 1

    def laplace(e, p, row):
        here = pl.ds(row, TILE)
        padded = pl.ds(pl.multiple_of(row + PAD, PAD), TILE)
        tall = st[e, p, pl.ds(row, TILE + 2 * PAD), :]
        mid = tall[PAD:PAD + TILE]
        beside = tall[PAD + 1:PAD + 1 + TILE] + tall[PAD - 1:PAD - 1 + TILE]
        beside = beside + jnp.where(rightmost, 0.0, pltpu.roll(mid, nx - 1, 1))
        beside = beside + jnp.where(leftmost, 0.0, pltpu.roll(mid, 1, 1))
        above = st[e, p + 1, padded, :] if p + 1 < planes else halo[1, e, here, :]
        below = st[e, p - 1, padded, :] if p > 0 else halo[0, e, here, :]
        return mid, beside + above + below - 6.0 * mid

    def ship(which, source, target, m):
        at = pl.multiple_of((CHUNKS - 2 - 2 * m) * (1 - h) * rows + 2 * m * h * rows, PAD)
        for o in range(2):
            dest = base + 2 * s + o
            src = source.at[pl.ds(o * own, own), pl.ds(at, 2 * rows), :]
            dst = target.at[:, pl.ds(pl.multiple_of(h * half + at, PAD), 2 * rows), :]

            @pl.when(dest == me)
            def _():
                pltpu.make_async_copy(src, dst, out_recv).start()

            @pl.when(dest != me)
            def _():
                pltpu.make_async_remote_copy(
                    src_ref=src, dst_ref=dst, send_sem=out_send.at[o],
                    recv_sem=out_recv, device_id=(dest,), device_id_type=MESH,
                ).start()

    def stage(e, j):
        at = pl.multiple_of((CHUNKS - 1 - j) * (1 - h) * rows + j * h * rows, PAD)
        @pl.when(j == 0)
        def _():
            take_edge(e)

        if e == ITERS - 1:
            fed(1, j)

        def tile(t, carry):
            row = pl.multiple_of(at + t * TILE, TILE)
            here = pl.ds(row, TILE)
            padded = pl.ds(pl.multiple_of(row + PAD, PAD), TILE)
            for p in range(planes):
                mid, slope = laplace(e, p, row)
                if e < ITERS - 1:
                    sl[e, p, here, :] = slope
                    st[e + 1, p, padded, :] = mid + time_step * coef[p, here, :] * slope
                elif e == ITERS - 1:
                    c = coef[p, here, :]
                    resid = mid + time_step * c * slope - obs[p, here, :]
                    weighted = wgt[p, here, :] * resid
                    acc[...] += weighted * resid
                    aacc[p, here, :] = weighted
                    gacc[p, here, :] = time_step * weighted * slope
                    st[e + 1, p, padded, :] = c * weighted
                else:
                    lam = aacc[p, here, :] + time_step * slope
                    aacc[p, here, :] = lam
                    if e < exchanges - 1:
                        gacc[p, here, :] += time_step * lam * sl[exchanges - 2 - e, p, here, :]
                        st[e + 1, p, padded, :] = coef[p, here, :] * lam
            return carry

        lax.fori_loop(0, rows // TILE, tile, 0)
        if e < exchanges - 1:
            @pl.when(j == 0)
            def _():
                stage_edge(e + 1)

            send(e + 1, at, j)

            @pl.when(j == 0)
            def _():
                edge_copy(e + 1).start()

    def exchange(r):
        return pltpu.make_async_remote_copy(
            src_ref=part.at[2 * r], dst_ref=part.at[2 * r + 1],
            send_sem=psend_sem, recv_sem=precv_sem.at[r],
            device_id=(sums[r],), device_id_type=MESH,
        )

    def across(o):
        return pltpu.make_async_remote_copy(
            src_ref=part.at[2 * rounds - 2], dst_ref=part.at[2 * rounds - 1],
            send_sem=psend_sem, recv_sem=precv_sem.at[rounds - 1],
            device_id=(base + 2 * (1 - h) + o,), device_id_type=MESH,
        )

    def total_round(r):
        if r == 0:
            whole = acc[...]
            narrow = whole[:, 0:128]
            for i in range(1, nx // 128):
                narrow = narrow + whole[:, 128 * i:128 * i + 128]
            part[0] = narrow
        else:
            exchange(r - 1).wait_recv()
            part[2 * r] = part[2 * r - 2] + part[2 * r - 1]
        if r < rounds - 1:
            exchange(r).start()
        else:
            @pl.when(free)
            def _():
                across(0).start()
                across(1).start()

    summed = CHUNKS + ITERS - 1
    ticks = CHUNKS + exchanges

    def tick(t, carry):
        @pl.when(t < CHUNKS)
        def _():
            at = pl.multiple_of((CHUNKS - 1 - t) * (1 - h) * rows + t * h * rows, PAD)
            fed(0, t)

            @pl.when(t == 0)
            def _():
                stage_edge(0)
                edge_copy(0).start()

            send(0, at, t)

        for e in range(exchanges):
            j = t - 1 - e
            if e % GROUP == 0:
                receive(e // GROUP, t)

            @pl.when((j >= 0) & (j < CHUNKS))
            def _():
                stage(e, j)

        @pl.when(t + 3 < CHUNKS)
        def _():
            feed(0, t + 3)
            feed(1, t + 3)

        late = t + 2 - ITERS + 1

        @pl.when((late >= 0) & (late < CHUNKS))
        def _():
            feed(2, late)
            feed(3, late)

        for which, source, target in ((0, gacc, grad_out), (1, aacc, adj_out)):
            early, since = t - SHIP - which, t - exchanges - which

            @pl.when((early >= 0) & (early <= SHIP - exchanges) & (early < CHUNKS // 2))
            def _():
                ship(which, source, target, early)

            @pl.when((since % 2 == 0) & (since // 2 > SHIP - exchanges) & (since // 2 < CHUNKS // 2))
            def _():
                ship(which, source, target, since // 2)

        for r in range(min(rounds, ticks - summed)):
            @pl.when(t == summed + r)
            def _():
                total_round(r)

        return carry

    lax.fori_loop(0, ticks, tick, 0)
    for r in range(ticks - summed, rounds):
        total_round(r)

    across(0).wait_recv()
    whole = part[2 * rounds - 2] + part[2 * rounds - 1]
    whole = jnp.sum(jnp.sum(whole, axis=1, keepdims=True), axis=0, keepdims=True)
    misfit_out[...] = jnp.sqrt(jnp.broadcast_to(whole, (8, 128)) / cells + 1e-06)

    slabs = st.at[pl.ds(0, 2), :, pl.ds(0, half), :]
    await_copy(slabs, out_recv)
    for o in range(2):
        @pl.when(base + 2 * s + o != me)
        def _():
            await_copy(coef, out_send.at[o])
    for to in range(2):
        @pl.when(base + 2 * to + q // 2 != me)
        def _():
            await_copy(slabs, in_send.at[to])

    @pl.when(has_hi)
    def _():
        await_copy(halo.at[0], halo_send.at[0])

    @pl.when(has_lo)
    def _():
        await_copy(halo.at[1], halo_send.at[1])

    await_copy(edge_out, edge_send)

    @pl.when(free)
    def _():
        await_copy(part.at[pl.ds(0, rounds + 1)], psend_sem)

    @pl.when(jnp.logical_not(free))
    def _():
        await_copy(part.at[pl.ds(0, rounds - 1)], psend_sem)


def finish(grad, adj, misfit, grad_out, adj_out, misfit_out, scaled, sem):
    own, ny, nx = grad.shape
    scale = misfit[...]
    misfit_out[...] = scale[0:1, 0:1]
    inverse = 1.0 / scale
    wide = jnp.concatenate([inverse] * (nx // 128), axis=1)
    for which, (source, target) in enumerate(((grad, grad_out), (adj, adj_out))):
        for p in range(own):
            def piece(i, carry):
                at = pl.multiple_of(i * PIECE, PIECE)
                for r in range(PIECE // TILE):
                    row = pl.multiple_of(at + r * TILE, TILE)
                    scaled[which, p, pl.ds(row, TILE), :] = source[p, pl.ds(row, TILE), :] * wide
                here = pl.ds(at, PIECE)
                pltpu.make_async_copy(scaled.at[which, p, here, :], target.at[p, here, :], sem).start()
                return carry

            lax.fori_loop(0, ny // PIECE, piece, 0)
    pltpu.make_async_copy(scaled, scaled, sem).wait()


def solution(mesh):
    n = mesh.shape["gz"]
    rounds = n.bit_length() - 1

    def on_device(coefficient, initial_field, observed, misfit_weight):
        own, ny, nx = coefficient.shape
        planes, half = 2 * own, ny // 2
        slab = jax.ShapeDtypeStruct(coefficient.shape, jnp.float32)
        exchanges = 2 * ITERS
        block = pltpu.VMEM((planes, half, nx), jnp.float32)
        edge = pltpu.VMEM((exchanges, planes, nx), jnp.float32)
        dma = pltpu.SemaphoreType.DMA
        grad, adj, misfit = pl.pallas_call(
            functools.partial(kernel, n, rounds, float(n * own * ny * nx)),
            out_shape=(slab, slab, jax.ShapeDtypeStruct((8, 128), jnp.float32)),
            in_specs=[pl.BlockSpec(memory_space=pl.ANY)] * 4,
            out_specs=[pl.BlockSpec(memory_space=pl.ANY)] * 2 + [pl.BlockSpec(memory_space=pltpu.VMEM)],
            scratch_shapes=[
                pltpu.VMEM((exchanges, planes, half + 2 * PAD, nx), jnp.float32),
                pltpu.VMEM((ITERS - 1, planes, half, nx), jnp.float32),
                pltpu.VMEM((2, exchanges, half, nx), jnp.float32),
                block, block, block, block, block,
                pltpu.VMEM((TILE, nx), jnp.float32),
                pltpu.VMEM((2 * rounds, 8, 128), jnp.float32),
                edge, edge,
                dma((2,)), dma((2, SLOTS)),
                dma((2,)), dma((exchanges // GROUP, RING)),
                dma, dma((2,)),
                dma((2,)), dma,
                dma, dma((rounds,)),
                pltpu.VMEM((2, own, half // CHUNKS, nx), jnp.float32), dma,
            ],
            compiler_params=pltpu.CompilerParams(
                collective_id=0, has_side_effects=True, vmem_limit_bytes=48 * 1024 * 1024
            ),
        )(coefficient, initial_field, observed, misfit_weight)
        vmem = pl.BlockSpec(memory_space=pltpu.VMEM)
        grad, adj, misfit = pl.pallas_call(
            finish,
            out_shape=(slab, slab, jax.ShapeDtypeStruct((1, 1), jnp.float32)),
            in_specs=[vmem] * 3,
            out_specs=[pl.BlockSpec(memory_space=pltpu.HBM)] * 2 + [vmem],
            scratch_shapes=[pltpu.VMEM((2, *coefficient.shape), jnp.float32), dma],
            compiler_params=pltpu.CompilerParams(vmem_limit_bytes=6 * 1024 * 1024),
        )(grad, adj, misfit)
        return grad, adj, misfit.reshape(())

    placed = P("gz", None, None)
    return jax.shard_map(
        on_device,
        mesh=mesh,
        in_specs=(placed,) * 4,
        out_specs=(placed, placed, P()),
        check_vma=False,
    )
```

```python
import functools

import jax
import jax.numpy as jnp
from jax import lax
from jax.experimental import pallas as pl
from jax.experimental.pallas import tpu as pltpu
from jax.sharding import PartitionSpec as P

ITERS = 4
time_step = 0.125
MESH = pl.DeviceIdType.MESH
PAD = 8
TILE = 8
CHUNKS = 16
RING = 4
GROUP = 4
SLOTS = 8
PIECE = 128
SHIP = 13
SLOW = 2


def kernel(n, rounds, cells, coef_hbm, init_hbm, obs_hbm, wgt_hbm, grad_out, adj_out, misfit_out,
           st, sl, halo, coef, obs, wgt, gacc, aacc, acc, part, edge_out, edge_in,
           in_send, in_recv, halo_send, halo_recv, edge_send, edge_recv,
           out_send, out_recv, psend_sem, precv_sem, first, first_sem):
    own, ny, nx = coef_hbm.shape
    planes, half = 2 * own, ny // 2
    rows = half // CHUNKS
    exchanges = 2 * ITERS
    me = lax.axis_index("gz")
    q = me % 4
    base = me - q
    h, s = q // 2, q % 2
    lower, upper = me - 3 + 2 * s, me + 1 + 2 * s
    mate = me + 2 - 4 * h
    has_lo = lower >= 0
    has_hi = upper < n
    partners = []
    for r in range(rounds):
        bit = 1 << r
        partners.append(me + bit * (1 - 2 * ((me // bit) % 2)))
    sums = [partners[0]] + partners[2:]
    free = s == h

    hbm = (init_hbm, coef_hbm, obs_hbm, wgt_hbm)
    held = (None, coef, obs, wgt)
    barrier = pltpu.get_barrier_semaphore()

    def greet(device):
        pl.semaphore_signal(barrier, inc=1, device_id=(device,), device_id_type=MESH)

    below, beyond = base > 0, base + 4 < n
    middle = (q == 1) | (q == 2)

    @pl.when(middle)
    def _():
        greet(base + jnp.where(q == 1, 3, 0))

    greet(base + jnp.where(middle, 3 - q, 1 + q // 3))

    @pl.when((h == s) & jnp.where(h == 0, below, beyond))
    def _():
        greet(me - 3 + 6 * h)

    @pl.when(middle & jnp.where(h == 0, beyond, below))
    def _():
        greet(me + 4 - 8 * h)

    for array in range(2):
        src = hbm[array].at[:, pl.ds(pl.multiple_of(half - h * rows, PAD), rows), :]
        pltpu.make_async_copy(src, first.at[array], first_sem).start()


    zero_rows = jnp.zeros((PAD, nx), jnp.float32)
    outer = pl.multiple_of(h * (PAD + half), PAD)
    inner = pl.multiple_of((1 - h) * (PAD + half), PAD)

    for central in (False, True):
        for sides in range(3 if central else 1):
            count = below.astype(jnp.int32) + beyond.astype(jnp.int32)

            @pl.when(middle & (count == sides) if central else jnp.logical_not(middle))
            def _():
                pl.semaphore_wait(barrier, 2 + sides if central else 1)

    def place(side_half, j):
        return j if side_half == 1 else CHUNKS - 1 - j

    def feed(array, j):
        for to in range(2):
            dest = base + 2 * to + q // 2
            row = place(to, j) * rows
            slot = pl.ds(s * own, own)
            if array == 0:
                src = init_hbm.at[:, pl.ds(pl.multiple_of(to * half + row, PAD), rows), :]
                dst = st.at[0, slot, pl.ds(pl.multiple_of(PAD + row, PAD), rows), :]
            else:
                src = hbm[array].at[:, pl.ds(pl.multiple_of(to * half + row, PAD), rows), :]
                dst = held[array].at[slot, pl.ds(pl.multiple_of(row, PAD), rows), :]
            arrived = in_recv.at[array // 2, j % SLOTS]
            distant = dest != me
            if isinstance(j, int) and j == 0:
                across_chips = q // 2 != to
                distant = distant & (q // 2 == to)

                @pl.when(across_chips)
                def _():
                    pltpu.make_async_remote_copy(
                        src_ref=first.at[array], dst_ref=dst, send_sem=in_send.at[to], recv_sem=arrived,
                        device_id=(dest,), device_id_type=MESH,
                    ).start()

            @pl.when(dest == me)
            def _():
                pltpu.make_async_copy(src, dst, arrived).start()

            @pl.when(distant)
            def _():
                pltpu.make_async_remote_copy(
                    src_ref=src, dst_ref=dst, send_sem=in_send.at[to], recv_sem=arrived,
                    device_id=(dest,), device_id_type=MESH,
                ).start()

    def await_copy(ref, sem):
        pltpu.make_async_copy(ref, ref, sem).wait()

    def fed(kind, j):
        await_copy(st.at[pl.ds(0, 2), :, pl.ds(0, rows), :], in_recv.at[kind, j % SLOTS])

    await_copy(first, first_sem)
    for j in range(3):
        feed(0, j)
        feed(1, j)

    def clear_pad(e, carry):
        for p in range(planes):
            st[e, p, pl.ds(outer, PAD), :] = zero_rows
        return carry

    lax.fori_loop(0, exchanges, clear_pad, 0)

    def clear_halo(side):
        def clear(i, carry):
            e = i // (half // PAD)
            row = pl.multiple_of((i % (half // PAD)) * PAD, PAD)
            halo[side, e, pl.ds(row, PAD), :] = zero_rows
            return carry

        lax.fori_loop(0, exchanges * (half // PAD), clear, 0)

    @pl.when(jnp.logical_not(has_lo))
    def _():
        clear_halo(0)

    @pl.when(jnp.logical_not(has_hi))
    def _():
        clear_halo(1)

    acc[...] = jnp.zeros_like(acc)
    def send(e, at, j):
        here = pl.ds(at, rows)
        padded = pl.ds(pl.multiple_of(PAD + at, PAD), rows)

        def copy(side, device):
            pltpu.make_async_remote_copy(
                src_ref=st.at[e, (planes - 1) * (1 - side), padded, :],
                dst_ref=halo.at[side, e, here, :],
                send_sem=halo_send.at[side], recv_sem=halo_recv.at[e // GROUP, (j + e + 1) % RING],
                device_id=(device,), device_id_type=MESH,
            ).start()

        @pl.when(has_hi)
        def _():
            copy(0, upper)

        @pl.when(has_lo)
        def _():
            copy(1, lower)

    def receive(group, t):
        first_stage = group * GROUP
        count = jnp.minimum(first_stage + GROUP, t) - jnp.maximum(first_stage, t - CHUNKS)
        arrived = halo_recv.at[group, t % RING]
        for stages in range(1, GROUP + 1):
            for sides in (1, 2):
                @pl.when((count == stages) & ((has_lo & has_hi) == (sides == 2)))
                def _():
                    await_copy(halo.at[pl.ds(0, sides), pl.ds(0, stages), pl.ds(0, rows), :], arrived)

    def edge_copy(e):
        return pltpu.make_async_remote_copy(
            src_ref=edge_out.at[e], dst_ref=edge_in.at[e],
            send_sem=edge_send, recv_sem=edge_recv.at[e % 2],
            device_id=(mate,), device_id_type=MESH,
        )

    def stage_edge(e):
        at = pl.multiple_of(PAD + (1 - h) * (half - PAD), PAD)
        for p in range(planes):
            block = st[e, p, pl.ds(at, PAD), :]
            edge_out[e, p:p + 1, :] = jnp.where(h == 0, block[PAD - 1:PAD], block[0:1])

    def take_edge(e):
        edge_copy(e).wait_recv()
        for p in range(planes):
            st[e, p, pl.ds(inner, PAD), :] = jnp.broadcast_to(edge_in[e, p:p + 1, :], (PAD, nx))

    lane = lax.broadcasted_iota(jnp.int32, (TILE, nx), 1)
    leftmost = lane == 0
    rightmost = lane == nx - 1

    def laplace(e, p, row):
        here = pl.ds(row, TILE)
        padded = pl.ds(pl.multiple_of(row + PAD, PAD), TILE)
        tall = st[e, p, pl.ds(row, TILE + 2 * PAD), :]
        mid = tall[PAD:PAD + TILE]
        beside = tall[PAD + 1:PAD + 1 + TILE] + tall[PAD - 1:PAD - 1 + TILE]
        beside = beside + jnp.where(rightmost, 0.0, pltpu.roll(mid, nx - 1, 1))
        beside = beside + jnp.where(leftmost, 0.0, pltpu.roll(mid, 1, 1))
        above = st[e, p + 1, padded, :] if p + 1 < planes else halo[1, e, here, :]
        below = st[e, p - 1, padded, :] if p > 0 else halo[0, e, here, :]
        return mid, beside + above + below - 6.0 * mid

    def ship(which, source, target, m):
        at = pl.multiple_of((CHUNKS - 2 - 2 * m) * (1 - h) * rows + 2 * m * h * rows, PAD)
        for o in range(2):
            dest = base + 2 * s + o
            src = source.at[pl.ds(o * own, own), pl.ds(at, 2 * rows), :]
            dst = target.at[:, pl.ds(pl.multiple_of(h * half + at, PAD), 2 * rows), :]

            @pl.when(dest == me)
            def _():
                pltpu.make_async_copy(src, dst, out_recv).start()

            @pl.when(dest != me)
            def _():
                pltpu.make_async_remote_copy(
                    src_ref=src, dst_ref=dst, send_sem=out_send.at[o],
                    recv_sem=out_recv, device_id=(dest,), device_id_type=MESH,
                ).start()

    def stage(e, j):
        at = pl.multiple_of((CHUNKS - 1 - j) * (1 - h) * rows + j * h * rows, PAD)
        @pl.when(j == 0)
        def _():
            take_edge(e)

        if e == ITERS - 1:
            fed(1, j)

        def tile(t, carry):
            row = pl.multiple_of(at + t * TILE, TILE)
            here = pl.ds(row, TILE)
            padded = pl.ds(pl.multiple_of(row + PAD, PAD), TILE)
            for p in range(planes):
                mid, slope = laplace(e, p, row)
                if e < ITERS - 1:
                    sl[e, p, here, :] = slope
                    st[e + 1, p, padded, :] = mid + time_step * coef[p, here, :] * slope
                elif e == ITERS - 1:
                    c = coef[p, here, :]
                    resid = mid + time_step * c * slope - obs[p, here, :]
                    weighted = wgt[p, here, :] * resid
                    acc[...] += weighted * resid
                    aacc[p, here, :] = weighted
                    gacc[p, here, :] = time_step * weighted * slope
                    st[e + 1, p, padded, :] = c * weighted
                else:
                    lam = aacc[p, here, :] + time_step * slope
                    aacc[p, here, :] = lam
                    if e < exchanges - 1:
                        gacc[p, here, :] += time_step * lam * sl[exchanges - 2 - e, p, here, :]
                        st[e + 1, p, padded, :] = coef[p, here, :] * lam
            return carry

        lax.fori_loop(0, rows // TILE, tile, 0)
        if e < exchanges - 1:
            @pl.when(j == 0)
            def _():
                stage_edge(e + 1)

            send(e + 1, at, j)

            @pl.when(j == 0)
            def _():
                edge_copy(e + 1).start()

    def exchange(r):
        return pltpu.make_async_remote_copy(
            src_ref=part.at[2 * r], dst_ref=part.at[2 * r + 1],
            send_sem=psend_sem, recv_sem=precv_sem.at[r],
            device_id=(sums[r],), device_id_type=MESH,
        )

    def across(o):
        return pltpu.make_async_remote_copy(
            src_ref=part.at[2 * rounds - 2], dst_ref=part.at[2 * rounds - 1],
            send_sem=psend_sem, recv_sem=precv_sem.at[rounds - 1],
            device_id=(base + 2 * (1 - h) + o,), device_id_type=MESH,
        )

    def total_round(r):
        if r == 0:
            whole = acc[...]
            narrow = whole[:, 0:128]
            for i in range(1, nx // 128):
                narrow = narrow + whole[:, 128 * i:128 * i + 128]
            part[0] = narrow
        else:
            exchange(r - 1).wait_recv()
            part[2 * r] = part[2 * r - 2] + part[2 * r - 1]
        if r < rounds - 1:
            exchange(r).start()
        else:
            @pl.when(free)
            def _():
                across(0).start()
                across(1).start()

    summed = CHUNKS + ITERS - 1
    ticks = CHUNKS + exchanges

    def tick(t, carry):
        @pl.when(t < CHUNKS)
        def _():
            at = pl.multiple_of((CHUNKS - 1 - t) * (1 - h) * rows + t * h * rows, PAD)
            fed(0, t)

            @pl.when(t == 0)
            def _():
                stage_edge(0)
                edge_copy(0).start()

            send(0, at, t)

        for e in range(exchanges):
            j = t - 1 - e
            if e % GROUP == 0:
                receive(e // GROUP, t)

            @pl.when((j >= 0) & (j < CHUNKS))
            def _():
                stage(e, j)

        @pl.when(t + 3 < CHUNKS)
        def _():
            feed(0, t + 3)
            feed(1, t + 3)

        late = t + 2 - ITERS + 1

        @pl.when((late >= 0) & (late < CHUNKS))
        def _():
            feed(2, late)
            feed(3, late)

        for which, source, target in ((0, gacc, grad_out), (1, aacc, adj_out)):
            slow, m = t - SHIP - which, t - SHIP - SLOW
            final = CHUNKS // 2 - 1

            @pl.when((slow >= 0) & (slow < 2 * SLOW) & (slow % 2 == 0))
            def _():
                ship(which, source, target, slow // 2)

            @pl.when((m >= SLOW) & (m <= final - which))
            def _():
                ship(which, source, target, m)

            if which == 1:
                @pl.when(m == final + 1)
                def _():
                    ship(which, source, target, final)

        for r in range(min(rounds, ticks - summed)):
            @pl.when(t == summed + r)
            def _():
                total_round(r)

        return carry

    lax.fori_loop(0, ticks, tick, 0)
    for r in range(ticks - summed, rounds):
        total_round(r)

    across(0).wait_recv()
    whole = part[2 * rounds - 2] + part[2 * rounds - 1]
    whole = jnp.sum(jnp.sum(whole, axis=1, keepdims=True), axis=0, keepdims=True)
    misfit_out[...] = jnp.sqrt(jnp.broadcast_to(whole, (8, 128)) / cells + 1e-06)

    slabs = st.at[pl.ds(0, 2), :, pl.ds(0, half), :]
    await_copy(slabs, out_recv)
    for o in range(2):
        @pl.when(base + 2 * s + o != me)
        def _():
            await_copy(coef, out_send.at[o])
    for to in range(2):
        @pl.when(base + 2 * to + q // 2 != me)
        def _():
            await_copy(slabs, in_send.at[to])

    @pl.when(has_hi)
    def _():
        await_copy(halo.at[0], halo_send.at[0])

    @pl.when(has_lo)
    def _():
        await_copy(halo.at[1], halo_send.at[1])

    await_copy(edge_out, edge_send)

    @pl.when(free)
    def _():
        await_copy(part.at[pl.ds(0, rounds + 1)], psend_sem)

    @pl.when(jnp.logical_not(free))
    def _():
        await_copy(part.at[pl.ds(0, rounds - 1)], psend_sem)


def finish(grad, adj, misfit, grad_out, adj_out, misfit_out, scaled, sem):
    own, ny, nx = grad.shape
    scale = misfit[...]
    misfit_out[...] = scale[0:1, 0:1]
    inverse = 1.0 / scale
    wide = jnp.concatenate([inverse] * (nx // 128), axis=1)
    for which, (source, target) in enumerate(((grad, grad_out), (adj, adj_out))):
        for p in range(own):
            def piece(i, carry):
                at = pl.multiple_of(i * PIECE, PIECE)
                for r in range(PIECE // TILE):
                    row = pl.multiple_of(at + r * TILE, TILE)
                    scaled[which, p, pl.ds(row, TILE), :] = source[p, pl.ds(row, TILE), :] * wide
                here = pl.ds(at, PIECE)
                pltpu.make_async_copy(scaled.at[which, p, here, :], target.at[p, here, :], sem).start()
                return carry

            lax.fori_loop(0, ny // PIECE, piece, 0)
    pltpu.make_async_copy(scaled, scaled, sem).wait()


def solution(mesh):
    n = mesh.shape["gz"]
    rounds = n.bit_length() - 1

    def on_device(coefficient, initial_field, observed, misfit_weight):
        own, ny, nx = coefficient.shape
        planes, half = 2 * own, ny // 2
        slab = jax.ShapeDtypeStruct(coefficient.shape, jnp.float32)
        exchanges = 2 * ITERS
        block = pltpu.VMEM((planes, half, nx), jnp.float32)
        edge = pltpu.VMEM((exchanges, planes, nx), jnp.float32)
        dma = pltpu.SemaphoreType.DMA
        grad, adj, misfit = pl.pallas_call(
            functools.partial(kernel, n, rounds, float(n * own * ny * nx)),
            out_shape=(slab, slab, jax.ShapeDtypeStruct((8, 128), jnp.float32)),
            in_specs=[pl.BlockSpec(memory_space=pl.ANY)] * 4,
            out_specs=[pl.BlockSpec(memory_space=pl.ANY)] * 2 + [pl.BlockSpec(memory_space=pltpu.VMEM)],
            scratch_shapes=[
                pltpu.VMEM((exchanges, planes, half + 2 * PAD, nx), jnp.float32),
                pltpu.VMEM((ITERS - 1, planes, half, nx), jnp.float32),
                pltpu.VMEM((2, exchanges, half, nx), jnp.float32),
                block, block, block, block, block,
                pltpu.VMEM((TILE, nx), jnp.float32),
                pltpu.VMEM((2 * rounds, 8, 128), jnp.float32),
                edge, edge,
                dma((2,)), dma((2, SLOTS)),
                dma((2,)), dma((exchanges // GROUP, RING)),
                dma, dma((2,)),
                dma((2,)), dma,
                dma, dma((rounds,)),
                pltpu.VMEM((2, own, half // CHUNKS, nx), jnp.float32), dma,
            ],
            compiler_params=pltpu.CompilerParams(
                collective_id=0, has_side_effects=True, vmem_limit_bytes=48 * 1024 * 1024
            ),
        )(coefficient, initial_field, observed, misfit_weight)
        vmem = pl.BlockSpec(memory_space=pltpu.VMEM)
        grad, adj, misfit = pl.pallas_call(
            finish,
            out_shape=(slab, slab, jax.ShapeDtypeStruct((1, 1), jnp.float32)),
            in_specs=[vmem] * 3,
            out_specs=[pl.BlockSpec(memory_space=pltpu.HBM)] * 2 + [vmem],
            scratch_shapes=[pltpu.VMEM((2, *coefficient.shape), jnp.float32), dma],
            compiler_params=pltpu.CompilerParams(vmem_limit_bytes=6 * 1024 * 1024),
        )(grad, adj, misfit)
        return grad, adj, misfit.reshape(())

    placed = P("gz", None, None)
    return jax.shard_map(
        on_device,
        mesh=mesh,
        in_specs=(placed,) * 4,
        out_specs=(placed, placed, P()),
        check_vma=False,
    )
```

```python
import functools

import jax
import jax.numpy as jnp
from jax import lax
from jax.experimental import pallas as pl
from jax.experimental.pallas import tpu as pltpu
from jax.sharding import PartitionSpec as P

ITERS = 4
time_step = 0.125
MESH = pl.DeviceIdType.MESH
PAD = 8
TILE = 8
CHUNKS = 16
RING = 4
GROUP = 4
SLOTS = 8
PIECE = 128
SHIP = 13
SLOW = 2


def kernel(n, rounds, cells, coef_hbm, init_hbm, obs_hbm, wgt_hbm, grad_out, adj_out, misfit_out,
           st, sl, halo, coef, obs, wgt, gacc, aacc, acc, part, edge_out, edge_in,
           in_send, in_recv, halo_send, halo_recv, edge_send, edge_recv,
           out_send, out_recv, psend_sem, precv_sem, first, first_sem):
    own, ny, nx = coef_hbm.shape
    planes, half = 2 * own, ny // 2
    rows = half // CHUNKS
    exchanges = 2 * ITERS
    me = lax.axis_index("gz")
    q = me % 4
    base = me - q
    h, s = q // 2, q % 2
    lower, upper = me - 3 + 2 * s, me + 1 + 2 * s
    mate = me + 2 - 4 * h
    has_lo = lower >= 0
    has_hi = upper < n
    partners = []
    for r in range(rounds):
        bit = 1 << r
        partners.append(me + bit * (1 - 2 * ((me // bit) % 2)))
    sums = [partners[0]] + partners[2:]
    free = s == h
    ahead = h == 1

    hbm = (init_hbm, coef_hbm, obs_hbm, wgt_hbm)
    held = (None, coef, obs, wgt)
    barrier = pltpu.get_barrier_semaphore()

    def greet(device):
        pl.semaphore_signal(barrier, inc=1, device_id=(device,), device_id_type=MESH)

    below, beyond = base > 0, base + 4 < n
    middle = (q == 1) | (q == 2)

    @pl.when(middle)
    def _():
        greet(base + jnp.where(q == 1, 3, 0))

    greet(base + jnp.where(middle, 3 - q, 1 + q // 3))

    @pl.when((h == s) & jnp.where(h == 0, below, beyond))
    def _():
        greet(me - 3 + 6 * h)

    @pl.when(middle & jnp.where(h == 0, beyond, below))
    def _():
        greet(me + 4 - 8 * h)

    for array in range(2):
        src = hbm[array].at[:, pl.ds(pl.multiple_of(half - h * rows, PAD), rows), :]
        pltpu.make_async_copy(src, first.at[array], first_sem).start()


    zero_rows = jnp.zeros((PAD, nx), jnp.float32)
    outer = pl.multiple_of(h * (PAD + half), PAD)
    inner = pl.multiple_of((1 - h) * (PAD + half), PAD)

    for central in (False, True):
        for sides in range(3 if central else 1):
            count = below.astype(jnp.int32) + beyond.astype(jnp.int32)

            @pl.when(middle & (count == sides) if central else jnp.logical_not(middle))
            def _():
                pl.semaphore_wait(barrier, 2 + sides if central else 1)

    def place(side_half, j):
        return j if side_half == 1 else CHUNKS - 1 - j

    def feed(array, j):
        for to in range(2):
            dest = base + 2 * to + q // 2
            row = place(to, j) * rows
            slot = pl.ds(s * own, own)
            if array == 0:
                src = init_hbm.at[:, pl.ds(pl.multiple_of(to * half + row, PAD), rows), :]
                dst = st.at[0, slot, pl.ds(pl.multiple_of(PAD + row, PAD), rows), :]
            else:
                src = hbm[array].at[:, pl.ds(pl.multiple_of(to * half + row, PAD), rows), :]
                dst = held[array].at[slot, pl.ds(pl.multiple_of(row, PAD), rows), :]
            arrived = in_recv.at[array // 2, j % SLOTS]
            distant = dest != me
            if isinstance(j, int) and j == 0:
                across_chips = q // 2 != to
                distant = distant & (q // 2 == to)

                @pl.when(across_chips)
                def _():
                    pltpu.make_async_remote_copy(
                        src_ref=first.at[array], dst_ref=dst, send_sem=in_send.at[to], recv_sem=arrived,
                        device_id=(dest,), device_id_type=MESH,
                    ).start()

            @pl.when(dest == me)
            def _():
                pltpu.make_async_copy(src, dst, arrived).start()

            @pl.when(distant)
            def _():
                pltpu.make_async_remote_copy(
                    src_ref=src, dst_ref=dst, send_sem=in_send.at[to], recv_sem=arrived,
                    device_id=(dest,), device_id_type=MESH,
                ).start()

    def await_copy(ref, sem):
        pltpu.make_async_copy(ref, ref, sem).wait()

    def fed(kind, j):
        await_copy(st.at[pl.ds(0, 2), :, pl.ds(0, rows), :], in_recv.at[kind, j % SLOTS])

    await_copy(first, first_sem)
    for j in range(3):
        feed(0, j)
        feed(1, j)

    def clear_pad(e, carry):
        for p in range(planes):
            st[e, p, pl.ds(outer, PAD), :] = zero_rows
        return carry

    lax.fori_loop(0, exchanges, clear_pad, 0)

    def clear_halo(side):
        def clear(i, carry):
            e = i // (half // PAD)
            row = pl.multiple_of((i % (half // PAD)) * PAD, PAD)
            halo[side, e, pl.ds(row, PAD), :] = zero_rows
            return carry

        lax.fori_loop(0, exchanges * (half // PAD), clear, 0)

    @pl.when(jnp.logical_not(has_lo))
    def _():
        clear_halo(0)

    @pl.when(jnp.logical_not(has_hi))
    def _():
        clear_halo(1)

    acc[...] = jnp.zeros_like(acc)
    def send(e, at, j):
        here = pl.ds(at, rows)
        padded = pl.ds(pl.multiple_of(PAD + at, PAD), rows)

        def copy(side, device):
            pltpu.make_async_remote_copy(
                src_ref=st.at[e, (planes - 1) * (1 - side), padded, :],
                dst_ref=halo.at[side, e, here, :],
                send_sem=halo_send.at[side], recv_sem=halo_recv.at[e // GROUP, (j + e + 1) % RING],
                device_id=(device,), device_id_type=MESH,
            ).start()

        @pl.when(has_hi)
        def _():
            copy(0, upper)

        @pl.when(has_lo)
        def _():
            copy(1, lower)

    def receive(group, t):
        first_stage = group * GROUP
        count = jnp.minimum(first_stage + GROUP, t) - jnp.maximum(first_stage, t - CHUNKS)
        arrived = halo_recv.at[group, t % RING]
        for stages in range(1, GROUP + 1):
            for sides in (1, 2):
                @pl.when((count == stages) & ((has_lo & has_hi) == (sides == 2)))
                def _():
                    await_copy(halo.at[pl.ds(0, sides), pl.ds(0, stages), pl.ds(0, rows), :], arrived)

    def edge_copy(e):
        return pltpu.make_async_remote_copy(
            src_ref=edge_out.at[e], dst_ref=edge_in.at[e],
            send_sem=edge_send, recv_sem=edge_recv.at[e % 2],
            device_id=(mate,), device_id_type=MESH,
        )

    def stage_edge(e):
        at = pl.multiple_of(PAD + (1 - h) * (half - PAD), PAD)
        for p in range(planes):
            block = st[e, p, pl.ds(at, PAD), :]
            edge_out[e, p:p + 1, :] = jnp.where(h == 0, block[PAD - 1:PAD], block[0:1])

    def take_edge(e):
        edge_copy(e).wait_recv()
        for p in range(planes):
            st[e, p, pl.ds(inner, PAD), :] = jnp.broadcast_to(edge_in[e, p:p + 1, :], (PAD, nx))

    lane = lax.broadcasted_iota(jnp.int32, (TILE, nx), 1)
    leftmost = lane == 0
    rightmost = lane == nx - 1

    def laplace(e, p, row):
        here = pl.ds(row, TILE)
        padded = pl.ds(pl.multiple_of(row + PAD, PAD), TILE)
        tall = st[e, p, pl.ds(row, TILE + 2 * PAD), :]
        mid = tall[PAD:PAD + TILE]
        beside = tall[PAD + 1:PAD + 1 + TILE] + tall[PAD - 1:PAD - 1 + TILE]
        beside = beside + jnp.where(rightmost, 0.0, pltpu.roll(mid, nx - 1, 1))
        beside = beside + jnp.where(leftmost, 0.0, pltpu.roll(mid, 1, 1))
        above = st[e, p + 1, padded, :] if p + 1 < planes else halo[1, e, here, :]
        below = st[e, p - 1, padded, :] if p > 0 else halo[0, e, here, :]
        return mid, beside + above + below - 6.0 * mid

    def ship(which, source, target, m):
        at = pl.multiple_of((CHUNKS - 2 - 2 * m) * (1 - h) * rows + 2 * m * h * rows, PAD)
        for o in range(2):
            dest = base + 2 * s + o
            src = source.at[pl.ds(o * own, own), pl.ds(at, 2 * rows), :]
            dst = target.at[:, pl.ds(pl.multiple_of(h * half + at, PAD), 2 * rows), :]

            @pl.when(dest == me)
            def _():
                pltpu.make_async_copy(src, dst, out_recv).start()

            @pl.when(dest != me)
            def _():
                pltpu.make_async_remote_copy(
                    src_ref=src, dst_ref=dst, send_sem=out_send.at[o],
                    recv_sem=out_recv, device_id=(dest,), device_id_type=MESH,
                ).start()

    def stage(e, j):
        at = pl.multiple_of((CHUNKS - 1 - j) * (1 - h) * rows + j * h * rows, PAD)
        @pl.when(j == 0)
        def _():
            take_edge(e)

        if e == ITERS - 1:
            fed(1, j)

        def tile(t, carry):
            row = pl.multiple_of(at + t * TILE, TILE)
            here = pl.ds(row, TILE)
            padded = pl.ds(pl.multiple_of(row + PAD, PAD), TILE)
            for p in range(planes):
                mid, slope = laplace(e, p, row)
                if e < ITERS - 1:
                    sl[e, p, here, :] = slope
                    st[e + 1, p, padded, :] = mid + time_step * coef[p, here, :] * slope
                elif e == ITERS - 1:
                    c = coef[p, here, :]
                    resid = mid + time_step * c * slope - obs[p, here, :]
                    weighted = wgt[p, here, :] * resid
                    acc[...] += weighted * resid
                    aacc[p, here, :] = weighted
                    gacc[p, here, :] = time_step * weighted * slope
                    st[e + 1, p, padded, :] = c * weighted
                else:
                    lam = aacc[p, here, :] + time_step * slope
                    aacc[p, here, :] = lam
                    if e < exchanges - 1:
                        gacc[p, here, :] += time_step * lam * sl[exchanges - 2 - e, p, here, :]
                        st[e + 1, p, padded, :] = coef[p, here, :] * lam
            return carry

        lax.fori_loop(0, rows // TILE, tile, 0)
        if e < exchanges - 1:
            @pl.when(j == 0)
            def _():
                stage_edge(e + 1)

            send(e + 1, at, j)

            @pl.when(j == 0)
            def _():
                edge_copy(e + 1).start()

    def exchange(r):
        return pltpu.make_async_remote_copy(
            src_ref=part.at[2 * r], dst_ref=part.at[2 * r + 1],
            send_sem=psend_sem, recv_sem=precv_sem.at[r],
            device_id=(sums[r],), device_id_type=MESH,
        )

    def across(o):
        return pltpu.make_async_remote_copy(
            src_ref=part.at[2 * rounds - 2], dst_ref=part.at[2 * rounds - 1],
            send_sem=psend_sem, recv_sem=precv_sem.at[rounds - 1],
            device_id=(base + 2 * (1 - h) + o,), device_id_type=MESH,
        )

    def total_round(r):
        if r == 0:
            whole = acc[...]
            narrow = whole[:, 0:128]
            for i in range(1, nx // 128):
                narrow = narrow + whole[:, 128 * i:128 * i + 128]
            part[0] = narrow
        else:
            exchange(r - 1).wait_recv()
            part[2 * r] = part[2 * r - 2] + part[2 * r - 1]
        if r < rounds - 1:
            exchange(r).start()
        else:
            @pl.when(free)
            def _():
                across(0).start()
                across(1).start()

    summed = CHUNKS + ITERS - 1
    ticks = CHUNKS + exchanges

    def tick(t, carry):
        @pl.when(t < CHUNKS)
        def _():
            at = pl.multiple_of((CHUNKS - 1 - t) * (1 - h) * rows + t * h * rows, PAD)
            fed(0, t)

            @pl.when(t == 0)
            def _():
                stage_edge(0)
                edge_copy(0).start()

            send(0, at, t)

        for e in range(exchanges):
            j = t - 1 - e
            if e % GROUP == 0:
                receive(e // GROUP, t)

            @pl.when((j >= 0) & (j < CHUNKS))
            def _():
                stage(e, j)

        @pl.when(t + 3 < CHUNKS)
        def _():
            feed(0, t + 3)
            feed(1, t + 3)

        late = t + 2 - ITERS + 1

        late = jnp.where(ahead & (t == 0), 0, late)

        @pl.when((late >= 0) & (late < CHUNKS) & jnp.logical_not(ahead & (t == 1)))
        def _():
            feed(2, late)
            feed(3, late)

        for which, source, target in ((0, gacc, grad_out), (1, aacc, adj_out)):
            slow, m = t - SHIP - which, t - SHIP - SLOW
            final = CHUNKS // 2 - 1

            @pl.when((slow >= 0) & (slow < 2 * SLOW) & (slow % 2 == 0))
            def _():
                ship(which, source, target, slow // 2)

            @pl.when((m >= SLOW) & (m <= final - which))
            def _():
                ship(which, source, target, m)

            if which == 1:
                @pl.when(m == final + 1)
                def _():
                    ship(which, source, target, final)

        for r in range(min(rounds, ticks - summed)):
            @pl.when(t == summed + r)
            def _():
                total_round(r)

        return carry

    lax.fori_loop(0, ticks, tick, 0)
    for r in range(ticks - summed, rounds):
        total_round(r)

    across(0).wait_recv()
    whole = part[2 * rounds - 2] + part[2 * rounds - 1]
    whole = jnp.sum(jnp.sum(whole, axis=1, keepdims=True), axis=0, keepdims=True)
    misfit_out[...] = jnp.sqrt(jnp.broadcast_to(whole, (8, 128)) / cells + 1e-06)

    slabs = st.at[pl.ds(0, 2), :, pl.ds(0, half), :]
    for to in range(2):
        @pl.when(base + 2 * to + q // 2 != me)
        def _():
            await_copy(slabs, in_send.at[to])

    @pl.when(has_hi)
    def _():
        await_copy(halo.at[0], halo_send.at[0])

    @pl.when(has_lo)
    def _():
        await_copy(halo.at[1], halo_send.at[1])

    await_copy(edge_out, edge_send)

    @pl.when(free)
    def _():
        await_copy(part.at[pl.ds(0, rounds + 1)], psend_sem)

    @pl.when(jnp.logical_not(free))
    def _():
        await_copy(part.at[pl.ds(0, rounds - 1)], psend_sem)

    for o in range(2):
        @pl.when(base + 2 * s + o != me)
        def _():
            await_copy(coef, out_send.at[o])

    await_copy(slabs, out_recv)


def finish(grad, adj, misfit, grad_out, adj_out, misfit_out, scaled, sem):
    own, ny, nx = grad.shape
    scale = misfit[...]
    misfit_out[...] = scale[0:1, 0:1]
    inverse = 1.0 / scale
    wide = jnp.concatenate([inverse] * (nx // 128), axis=1)
    for which, (source, target) in enumerate(((grad, grad_out), (adj, adj_out))):
        for p in range(own):
            def piece(i, carry):
                at = pl.multiple_of(i * PIECE, PIECE)
                for r in range(PIECE // TILE):
                    row = pl.multiple_of(at + r * TILE, TILE)
                    scaled[which, p, pl.ds(row, TILE), :] = source[p, pl.ds(row, TILE), :] * wide
                here = pl.ds(at, PIECE)
                pltpu.make_async_copy(scaled.at[which, p, here, :], target.at[p, here, :], sem).start()
                return carry

            lax.fori_loop(0, ny // PIECE, piece, 0)
    pltpu.make_async_copy(scaled, scaled, sem).wait()


def solution(mesh):
    n = mesh.shape["gz"]
    rounds = n.bit_length() - 1

    def on_device(coefficient, initial_field, observed, misfit_weight):
        own, ny, nx = coefficient.shape
        planes, half = 2 * own, ny // 2
        slab = jax.ShapeDtypeStruct(coefficient.shape, jnp.float32)
        exchanges = 2 * ITERS
        block = pltpu.VMEM((planes, half, nx), jnp.float32)
        edge = pltpu.VMEM((exchanges, planes, nx), jnp.float32)
        dma = pltpu.SemaphoreType.DMA
        grad, adj, misfit = pl.pallas_call(
            functools.partial(kernel, n, rounds, float(n * own * ny * nx)),
            out_shape=(slab, slab, jax.ShapeDtypeStruct((8, 128), jnp.float32)),
            in_specs=[pl.BlockSpec(memory_space=pl.ANY)] * 4,
            out_specs=[pl.BlockSpec(memory_space=pl.ANY)] * 2 + [pl.BlockSpec(memory_space=pltpu.VMEM)],
            scratch_shapes=[
                pltpu.VMEM((exchanges, planes, half + 2 * PAD, nx), jnp.float32),
                pltpu.VMEM((ITERS - 1, planes, half, nx), jnp.float32),
                pltpu.VMEM((2, exchanges, half, nx), jnp.float32),
                block, block, block, block, block,
                pltpu.VMEM((TILE, nx), jnp.float32),
                pltpu.VMEM((2 * rounds, 8, 128), jnp.float32),
                edge, edge,
                dma((2,)), dma((2, SLOTS)),
                dma((2,)), dma((exchanges // GROUP, RING)),
                dma, dma((2,)),
                dma((2,)), dma,
                dma, dma((rounds,)),
                pltpu.VMEM((2, own, half // CHUNKS, nx), jnp.float32), dma,
            ],
            compiler_params=pltpu.CompilerParams(
                collective_id=0, has_side_effects=True, vmem_limit_bytes=48 * 1024 * 1024
            ),
        )(coefficient, initial_field, observed, misfit_weight)
        vmem = pl.BlockSpec(memory_space=pltpu.VMEM)
        grad, adj, misfit = pl.pallas_call(
            finish,
            out_shape=(slab, slab, jax.ShapeDtypeStruct((1, 1), jnp.float32)),
            in_specs=[vmem] * 3,
            out_specs=[pl.BlockSpec(memory_space=pltpu.HBM)] * 2 + [vmem],
            scratch_shapes=[pltpu.VMEM((2, *coefficient.shape), jnp.float32), dma],
            compiler_params=pltpu.CompilerParams(vmem_limit_bytes=6 * 1024 * 1024),
        )(grad, adj, misfit)
        return grad, adj, misfit.reshape(())

    placed = P("gz", None, None)
    return jax.shard_map(
        on_device,
        mesh=mesh,
        in_specs=(placed,) * 4,
        out_specs=(placed, placed, P()),
        check_vma=False,
    )
```

```python
import functools

import jax
import jax.numpy as jnp
from jax import lax
from jax.experimental import pallas as pl
from jax.experimental.pallas import tpu as pltpu
from jax.sharding import PartitionSpec as P

ITERS = 4
time_step = 0.125
MESH = pl.DeviceIdType.MESH
PAD = 8
TILE = 8
CHUNKS = 16
RING = 4
GROUP = 4
SLOTS = 8
PIECE = 64
SHIP = 13
SLOW = 2


def kernel(n, rounds, cells, coef_hbm, init_hbm, obs_hbm, wgt_hbm, grad_out, adj_out, misfit_out,
           st, sl, halo, coef, obs, wgt, gacc, aacc, acc, part, edge_out, edge_in,
           in_send, in_recv, halo_send, halo_recv, edge_send, edge_recv,
           out_send, out_recv, psend_sem, precv_sem, first, first_sem):
    own, ny, nx = coef_hbm.shape
    planes, half = 2 * own, ny // 2
    rows = half // CHUNKS
    exchanges = 2 * ITERS
    me = lax.axis_index("gz")
    q = me % 4
    base = me - q
    h, s = q // 2, q % 2
    lower, upper = me - 3 + 2 * s, me + 1 + 2 * s
    mate = me + 2 - 4 * h
    has_lo = lower >= 0
    has_hi = upper < n
    partners = []
    for r in range(rounds):
        bit = 1 << r
        partners.append(me + bit * (1 - 2 * ((me // bit) % 2)))
    sums = [partners[0]] + partners[2:]
    free = s == h
    ahead = h == 1

    hbm = (init_hbm, coef_hbm, obs_hbm, wgt_hbm)
    held = (None, coef, obs, wgt)
    barrier = pltpu.get_barrier_semaphore()

    def greet(device):
        pl.semaphore_signal(barrier, inc=1, device_id=(device,), device_id_type=MESH)

    below, beyond = base > 0, base + 4 < n
    middle = (q == 1) | (q == 2)

    @pl.when(middle)
    def _():
        greet(base + jnp.where(q == 1, 3, 0))

    greet(base + jnp.where(middle, 3 - q, 1 + q // 3))

    @pl.when((h == s) & jnp.where(h == 0, below, beyond))
    def _():
        greet(me - 3 + 6 * h)

    @pl.when(middle & jnp.where(h == 0, beyond, below))
    def _():
        greet(me + 4 - 8 * h)

    for array in range(2):
        src = hbm[array].at[:, pl.ds(pl.multiple_of(half - h * rows, PAD), rows), :]
        pltpu.make_async_copy(src, first.at[array], first_sem).start()


    zero_rows = jnp.zeros((PAD, nx), jnp.float32)
    outer = pl.multiple_of(h * (PAD + half), PAD)
    inner = pl.multiple_of((1 - h) * (PAD + half), PAD)

    for central in (False, True):
        for sides in range(3 if central else 1):
            count = below.astype(jnp.int32) + beyond.astype(jnp.int32)

            @pl.when(middle & (count == sides) if central else jnp.logical_not(middle))
            def _():
                pl.semaphore_wait(barrier, 2 + sides if central else 1)

    def place(side_half, j):
        return j if side_half == 1 else CHUNKS - 1 - j

    def feed(array, j):
        for to in range(2):
            dest = base + 2 * to + q // 2
            row = place(to, j) * rows
            slot = pl.ds(s * own, own)
            if array == 0:
                src = init_hbm.at[:, pl.ds(pl.multiple_of(to * half + row, PAD), rows), :]
                dst = st.at[0, slot, pl.ds(pl.multiple_of(PAD + row, PAD), rows), :]
            else:
                src = hbm[array].at[:, pl.ds(pl.multiple_of(to * half + row, PAD), rows), :]
                dst = held[array].at[slot, pl.ds(pl.multiple_of(row, PAD), rows), :]
            arrived = in_recv.at[array // 2, j % SLOTS]
            distant = dest != me
            if isinstance(j, int) and j == 0:
                across_chips = q // 2 != to
                distant = distant & (q // 2 == to)

                @pl.when(across_chips)
                def _():
                    pltpu.make_async_remote_copy(
                        src_ref=first.at[array], dst_ref=dst, send_sem=in_send.at[to], recv_sem=arrived,
                        device_id=(dest,), device_id_type=MESH,
                    ).start()

            @pl.when(dest == me)
            def _():
                pltpu.make_async_copy(src, dst, arrived).start()

            @pl.when(distant)
            def _():
                pltpu.make_async_remote_copy(
                    src_ref=src, dst_ref=dst, send_sem=in_send.at[to], recv_sem=arrived,
                    device_id=(dest,), device_id_type=MESH,
                ).start()

    def await_copy(ref, sem):
        pltpu.make_async_copy(ref, ref, sem).wait()

    def fed(kind, j):
        await_copy(st.at[pl.ds(0, 2), :, pl.ds(0, rows), :], in_recv.at[kind, j % SLOTS])

    await_copy(first, first_sem)
    for j in range(3):
        feed(0, j)
        feed(1, j)

    def clear_pad(e, carry):
        for p in range(planes):
            st[e, p, pl.ds(outer, PAD), :] = zero_rows
        return carry

    lax.fori_loop(0, exchanges, clear_pad, 0)

    def clear_halo(side):
        def clear(i, carry):
            e = i // (half // PAD)
            row = pl.multiple_of((i % (half // PAD)) * PAD, PAD)
            halo[side, e, pl.ds(row, PAD), :] = zero_rows
            return carry

        lax.fori_loop(0, exchanges * (half // PAD), clear, 0)

    @pl.when(jnp.logical_not(has_lo))
    def _():
        clear_halo(0)

    @pl.when(jnp.logical_not(has_hi))
    def _():
        clear_halo(1)

    acc[...] = jnp.zeros_like(acc)
    def send(e, at, j):
        here = pl.ds(at, rows)
        padded = pl.ds(pl.multiple_of(PAD + at, PAD), rows)

        def copy(side, device):
            pltpu.make_async_remote_copy(
                src_ref=st.at[e, (planes - 1) * (1 - side), padded, :],
                dst_ref=halo.at[side, e, here, :],
                send_sem=halo_send.at[side], recv_sem=halo_recv.at[e // GROUP, (j + e + 1) % RING],
                device_id=(device,), device_id_type=MESH,
            ).start()

        @pl.when(has_hi)
        def _():
            copy(0, upper)

        @pl.when(has_lo)
        def _():
            copy(1, lower)

    def receive(group, t):
        first_stage = group * GROUP
        count = jnp.minimum(first_stage + GROUP, t) - jnp.maximum(first_stage, t - CHUNKS)
        arrived = halo_recv.at[group, t % RING]
        for stages in range(1, GROUP + 1):
            for sides in (1, 2):
                @pl.when((count == stages) & ((has_lo & has_hi) == (sides == 2)))
                def _():
                    await_copy(halo.at[pl.ds(0, sides), pl.ds(0, stages), pl.ds(0, rows), :], arrived)

    def edge_copy(e):
        return pltpu.make_async_remote_copy(
            src_ref=edge_out.at[e], dst_ref=edge_in.at[e],
            send_sem=edge_send, recv_sem=edge_recv.at[e % 2],
            device_id=(mate,), device_id_type=MESH,
        )

    def stage_edge(e):
        at = pl.multiple_of(PAD + (1 - h) * (half - PAD), PAD)
        for p in range(planes):
            block = st[e, p, pl.ds(at, PAD), :]
            edge_out[e, p:p + 1, :] = jnp.where(h == 0, block[PAD - 1:PAD], block[0:1])

    def take_edge(e):
        edge_copy(e).wait_recv()
        for p in range(planes):
            st[e, p, pl.ds(inner, PAD), :] = jnp.broadcast_to(edge_in[e, p:p + 1, :], (PAD, nx))

    lane = lax.broadcasted_iota(jnp.int32, (TILE, nx), 1)
    leftmost = lane == 0
    rightmost = lane == nx - 1

    def laplace(e, p, row):
        here = pl.ds(row, TILE)
        padded = pl.ds(pl.multiple_of(row + PAD, PAD), TILE)
        tall = st[e, p, pl.ds(row, TILE + 2 * PAD), :]
        mid = tall[PAD:PAD + TILE]
        beside = tall[PAD + 1:PAD + 1 + TILE] + tall[PAD - 1:PAD - 1 + TILE]
        beside = beside + jnp.where(rightmost, 0.0, pltpu.roll(mid, nx - 1, 1))
        beside = beside + jnp.where(leftmost, 0.0, pltpu.roll(mid, 1, 1))
        above = st[e, p + 1, padded, :] if p + 1 < planes else halo[1, e, here, :]
        below = st[e, p - 1, padded, :] if p > 0 else halo[0, e, here, :]
        return mid, beside + above + below - 6.0 * mid

    def ship(which, source, target, m):
        at = pl.multiple_of((CHUNKS - 2 - 2 * m) * (1 - h) * rows + 2 * m * h * rows, PAD)
        for o in range(2):
            dest = base + 2 * s + o
            src = source.at[pl.ds(o * own, own), pl.ds(at, 2 * rows), :]
            dst = target.at[:, pl.ds(pl.multiple_of(h * half + at, PAD), 2 * rows), :]

            @pl.when(dest == me)
            def _():
                pltpu.make_async_copy(src, dst, out_recv).start()

            @pl.when(dest != me)
            def _():
                pltpu.make_async_remote_copy(
                    src_ref=src, dst_ref=dst, send_sem=out_send.at[o],
                    recv_sem=out_recv, device_id=(dest,), device_id_type=MESH,
                ).start()

    def stage(e, j):
        at = pl.multiple_of((CHUNKS - 1 - j) * (1 - h) * rows + j * h * rows, PAD)
        @pl.when(j == 0)
        def _():
            take_edge(e)

        if e == ITERS - 1:
            fed(1, j)

        def tile(t, carry):
            row = pl.multiple_of(at + t * TILE, TILE)
            here = pl.ds(row, TILE)
            padded = pl.ds(pl.multiple_of(row + PAD, PAD), TILE)
            for p in range(planes):
                mid, slope = laplace(e, p, row)
                if e < ITERS - 1:
                    sl[e, p, here, :] = slope
                    st[e + 1, p, padded, :] = mid + time_step * coef[p, here, :] * slope
                elif e == ITERS - 1:
                    c = coef[p, here, :]
                    resid = mid + time_step * c * slope - obs[p, here, :]
                    weighted = wgt[p, here, :] * resid
                    acc[...] += weighted * resid
                    aacc[p, here, :] = weighted
                    gacc[p, here, :] = time_step * weighted * slope
                    st[e + 1, p, padded, :] = c * weighted
                else:
                    lam = aacc[p, here, :] + time_step * slope
                    aacc[p, here, :] = lam
                    if e < exchanges - 1:
                        gacc[p, here, :] += time_step * lam * sl[exchanges - 2 - e, p, here, :]
                        st[e + 1, p, padded, :] = coef[p, here, :] * lam
            return carry

        lax.fori_loop(0, rows // TILE, tile, 0)
        if e < exchanges - 1:
            @pl.when(j == 0)
            def _():
                stage_edge(e + 1)

            send(e + 1, at, j)

            @pl.when(j == 0)
            def _():
                edge_copy(e + 1).start()

    def exchange(r):
        return pltpu.make_async_remote_copy(
            src_ref=part.at[2 * r], dst_ref=part.at[2 * r + 1],
            send_sem=psend_sem, recv_sem=precv_sem.at[r],
            device_id=(sums[r],), device_id_type=MESH,
        )

    def across(o):
        return pltpu.make_async_remote_copy(
            src_ref=part.at[2 * rounds - 2], dst_ref=part.at[2 * rounds - 1],
            send_sem=psend_sem, recv_sem=precv_sem.at[rounds - 1],
            device_id=(base + 2 * (1 - h) + o,), device_id_type=MESH,
        )

    def total_round(r):
        if r == 0:
            whole = acc[...]
            narrow = whole[:, 0:128]
            for i in range(1, nx // 128):
                narrow = narrow + whole[:, 128 * i:128 * i + 128]
            part[0] = narrow
        else:
            exchange(r - 1).wait_recv()
            part[2 * r] = part[2 * r - 2] + part[2 * r - 1]
        if r < rounds - 1:
            exchange(r).start()
        else:
            @pl.when(free)
            def _():
                across(0).start()
                across(1).start()

    summed = CHUNKS + ITERS - 1
    ticks = CHUNKS + exchanges

    def tick(t, carry):
        @pl.when(t < CHUNKS)
        def _():
            at = pl.multiple_of((CHUNKS - 1 - t) * (1 - h) * rows + t * h * rows, PAD)
            fed(0, t)

            @pl.when(t == 0)
            def _():
                stage_edge(0)
                edge_copy(0).start()

            send(0, at, t)

        for e in range(exchanges):
            j = t - 1 - e
            if e % GROUP == 0:
                receive(e // GROUP, t)

            @pl.when((j >= 0) & (j < CHUNKS))
            def _():
                stage(e, j)

        @pl.when(t + 3 < CHUNKS)
        def _():
            feed(0, t + 3)
            feed(1, t + 3)

        late = t + 2 - ITERS + 1

        late = jnp.where(ahead & (t == 0), 0, late)

        @pl.when((late >= 0) & (late < CHUNKS) & jnp.logical_not(ahead & (t == 1)))
        def _():
            feed(2, late)
            feed(3, late)

        for which, source, target in ((0, gacc, grad_out), (1, aacc, adj_out)):
            slow, m = t - SHIP - which, t - SHIP - SLOW
            final = CHUNKS // 2 - 1

            @pl.when((slow >= 0) & (slow < 2 * SLOW) & (slow % 2 == 0))
            def _():
                ship(which, source, target, slow // 2)

            @pl.when((m >= SLOW) & (m <= final - which))
            def _():
                ship(which, source, target, m)

            if which == 1:
                @pl.when(m == final + 1)
                def _():
                    ship(which, source, target, final)

        for r in range(min(rounds, ticks - summed)):
            @pl.when(t == summed + r)
            def _():
                total_round(r)

        return carry

    lax.fori_loop(0, ticks, tick, 0)
    for r in range(ticks - summed, rounds):
        total_round(r)

    across(0).wait_recv()
    whole = part[2 * rounds - 2] + part[2 * rounds - 1]
    whole = jnp.sum(jnp.sum(whole, axis=1, keepdims=True), axis=0, keepdims=True)
    misfit_out[...] = jnp.sqrt(jnp.broadcast_to(whole, (8, 128)) / cells + 1e-06)

    slabs = st.at[pl.ds(0, 2), :, pl.ds(0, half), :]
    for to in range(2):
        @pl.when(base + 2 * to + q // 2 != me)
        def _():
            await_copy(slabs, in_send.at[to])

    @pl.when(has_hi)
    def _():
        await_copy(halo.at[0], halo_send.at[0])

    @pl.when(has_lo)
    def _():
        await_copy(halo.at[1], halo_send.at[1])

    await_copy(edge_out, edge_send)

    @pl.when(free)
    def _():
        await_copy(part.at[pl.ds(0, rounds + 1)], psend_sem)

    @pl.when(jnp.logical_not(free))
    def _():
        await_copy(part.at[pl.ds(0, rounds - 1)], psend_sem)

    for o in range(2):
        @pl.when(base + 2 * s + o != me)
        def _():
            await_copy(coef, out_send.at[o])

    await_copy(slabs, out_recv)


def finish(grad, adj, misfit, grad_out, adj_out, misfit_out, scaled, sem):
    own, ny, nx = grad.shape
    scale = misfit[...]
    misfit_out[...] = scale[0:1, 0:1]
    inverse = 1.0 / scale
    wide = jnp.concatenate([inverse] * (nx // 128), axis=1)
    for which, (source, target) in enumerate(((grad, grad_out), (adj, adj_out))):
        for p in range(own):
            def piece(i, carry):
                at = pl.multiple_of(i * PIECE, PIECE)
                for r in range(PIECE // TILE):
                    row = pl.multiple_of(at + r * TILE, TILE)
                    scaled[which, p, pl.ds(row, TILE), :] = source[p, pl.ds(row, TILE), :] * wide
                here = pl.ds(at, PIECE)
                pltpu.make_async_copy(scaled.at[which, p, here, :], target.at[p, here, :], sem).start()
                return carry

            lax.fori_loop(0, ny // PIECE, piece, 0)
    pltpu.make_async_copy(scaled, scaled, sem).wait()


def solution(mesh):
    n = mesh.shape["gz"]
    rounds = n.bit_length() - 1

    def on_device(coefficient, initial_field, observed, misfit_weight):
        own, ny, nx = coefficient.shape
        planes, half = 2 * own, ny // 2
        slab = jax.ShapeDtypeStruct(coefficient.shape, jnp.float32)
        exchanges = 2 * ITERS
        block = pltpu.VMEM((planes, half, nx), jnp.float32)
        edge = pltpu.VMEM((exchanges, planes, nx), jnp.float32)
        dma = pltpu.SemaphoreType.DMA
        grad, adj, misfit = pl.pallas_call(
            functools.partial(kernel, n, rounds, float(n * own * ny * nx)),
            out_shape=(slab, slab, jax.ShapeDtypeStruct((8, 128), jnp.float32)),
            in_specs=[pl.BlockSpec(memory_space=pl.ANY)] * 4,
            out_specs=[pl.BlockSpec(memory_space=pl.ANY)] * 2 + [pl.BlockSpec(memory_space=pltpu.VMEM)],
            scratch_shapes=[
                pltpu.VMEM((exchanges, planes, half + 2 * PAD, nx), jnp.float32),
                pltpu.VMEM((ITERS - 1, planes, half, nx), jnp.float32),
                pltpu.VMEM((2, exchanges, half, nx), jnp.float32),
                block, block, block, block, block,
                pltpu.VMEM((TILE, nx), jnp.float32),
                pltpu.VMEM((2 * rounds, 8, 128), jnp.float32),
                edge, edge,
                dma((2,)), dma((2, SLOTS)),
                dma((2,)), dma((exchanges // GROUP, RING)),
                dma, dma((2,)),
                dma((2,)), dma,
                dma, dma((rounds,)),
                pltpu.VMEM((2, own, half // CHUNKS, nx), jnp.float32), dma,
            ],
            compiler_params=pltpu.CompilerParams(
                collective_id=0, has_side_effects=True, vmem_limit_bytes=48 * 1024 * 1024
            ),
        )(coefficient, initial_field, observed, misfit_weight)
        vmem = pl.BlockSpec(memory_space=pltpu.VMEM)
        grad, adj, misfit = pl.pallas_call(
            finish,
            out_shape=(slab, slab, jax.ShapeDtypeStruct((1, 1), jnp.float32)),
            in_specs=[vmem] * 3,
            out_specs=[pl.BlockSpec(memory_space=pltpu.HBM)] * 2 + [vmem],
            scratch_shapes=[pltpu.VMEM((2, *coefficient.shape), jnp.float32), dma],
            compiler_params=pltpu.CompilerParams(vmem_limit_bytes=6 * 1024 * 1024),
        )(grad, adj, misfit)
        return grad, adj, misfit.reshape(())

    placed = P("gz", None, None)
    return jax.shard_map(
        on_device,
        mesh=mesh,
        in_specs=(placed,) * 4,
        out_specs=(placed, placed, P()),
        check_vma=False,
    )
```
